256 devices in a mesh: first: 16 (over y, x), second: 16 (over z, core).
Axes of the slice: x: 4, y: 4, z: 8, core: 2. Of those that a mesh axis runs over, the one named last changes fastest.
Arguments:
- pair_state: bfloat16 [768, 768, 128], P('first', 'second'), may hold values from -6 to 6
- in_gain: float32 [128], replicated, may hold values from 0.25 to 1.75
- left_weight: bfloat16 [128, 128], replicated, may hold values from -0.5 to 0.5
- right_weight: bfloat16 [128, 128], replicated, may hold values from -0.5 to 0.5
- mid_gain: float32 [128], replicated, may hold values from 0.25 to 1.75
- out_weight: bfloat16 [128, 128], replicated, may hold values from -0.5 to 0.5
- out_gate: bfloat16 [128, 128], replicated, may hold values from -0.5 to 0.5
Outputs:
- triangle_out: bfloat16 [768, 768, 128], P('first', 'second')
The draws below stay inside these ranges and needn't reach their ends.
All inputs are finite; a program needn't handle non-finite values.
Results may differ from the reference program's by a relative error of at most 0.015.
Values may be sent and summed in bfloat16 or wider, within the bound.
A program may use at most 64 MiB of HBM per device.

```python
import jax
import jax.numpy as jnp
from jax import lax

RESIDUES = 768
PAIR_WIDTH = 128
MIX_WIDTH = 128


def shard_levels(own_key, extent, cuts, smallest, largest):
    def one(axis_at, parts):
        draws = jax.random.uniform(jax.random.fold_in(jax.random.fold_in(own_key, 6), axis_at), (parts,), jnp.float32, smallest / len(cuts), largest / len(cuts))
        return jnp.repeat(jnp.exp(draws), extent[axis_at] // parts).reshape((-1,) + (1,) * (len(extent) - axis_at - 1))

    factor_of = one(*cuts[0])
    for cut in cuts[1:]:
        factor_of = factor_of * one(*cut)
    return factor_of


def scatter_about(key, extent, scale, bound, split=(), kind=jnp.bfloat16):
    gain = shard_levels(key, extent, split, -0.22, 0.18) if split else 1.0
    values = jax.random.normal(key, extent, jnp.float32) * scale * gain
    return jnp.minimum(jnp.maximum(values, -bound), bound).astype(kind)


def setup_inputs(seed: int = 0) -> dict:
    arg_keys = jax.random.split(jax.random.key(seed), 8)
    return {
        "pair_state": scatter_about(arg_keys[0], (RESIDUES, RESIDUES, PAIR_WIDTH), 1.0, 6.0, ((0, 16), (1, 16))),
        "in_gain": jnp.clip(1.0 + 0.15 * jax.random.normal(arg_keys[1], (PAIR_WIDTH,), jnp.float32), 0.25, 1.75),
        "left_weight": scatter_about(arg_keys[2], (PAIR_WIDTH, MIX_WIDTH), PAIR_WIDTH ** -0.5, 0.5),
        "right_weight": scatter_about(arg_keys[3], (PAIR_WIDTH, MIX_WIDTH), PAIR_WIDTH ** -0.5, 0.5),
        "mid_gain": jnp.clip(1.0 + 0.15 * jax.random.normal(arg_keys[4], (MIX_WIDTH,), jnp.float32), 0.25, 1.75),
        "out_weight": scatter_about(arg_keys[5], (MIX_WIDTH, PAIR_WIDTH), MIX_WIDTH ** -0.5, 0.5),
        "out_gate": scatter_about(arg_keys[6], (PAIR_WIDTH, PAIR_WIDTH), PAIR_WIDTH ** -0.5, 0.5),
    }


def unit_channels(values, channel_gain):
    centred = values - lax.optimization_barrier(jnp.mean(values, axis=-1, keepdims=True))
    return centred * lax.rsqrt(lax.optimization_barrier(jnp.mean(centred * centred, axis=-1, keepdims=True)) + 1e-05) * channel_gain

def make_factors(pair_in, in_gain, left_weight, right_weight):
    ready = unit_channels(pair_in.astype(jnp.float32), in_gain).astype(jnp.bfloat16)
    ready = lax.optimization_barrier(ready)
    left = jnp.einsum('ijc,cd->ijd', ready.astype(jnp.float32), left_weight.astype(jnp.float32))
    right = jnp.einsum('ijc,cd->ijd', ready.astype(jnp.float32), right_weight.astype(jnp.float32))
    return (ready, left.astype(jnp.bfloat16), right.astype(jnp.bfloat16))

def finish_pair(mixed, ready, mid_gain, out_weight, out_gate):
    scaled = unit_channels(mixed.astype(jnp.float32), mid_gain).astype(jnp.bfloat16)
    scaled = lax.optimization_barrier(scaled)
    gate = jax.nn.sigmoid(jnp.einsum('ijc,cd->ijd', ready.astype(jnp.float32), out_gate.astype(jnp.float32)))
    return (jnp.einsum('ijd,dc->ijc', scaled.astype(jnp.float32), out_weight.astype(jnp.float32)) * gate).astype(jnp.bfloat16)

def reference(pair_state, in_gain, left_weight, right_weight, mid_gain, out_weight, out_gate):
    ready, left, right = make_factors(pair_state, in_gain, left_weight, right_weight)
    left, right = lax.optimization_barrier((left, right))

    def one_channel(pair_of):
        return (jnp.dot(pair_of[0], pair_of[1].T, preferred_element_type=jnp.float32) * RESIDUES ** (-0.5)).astype(jnp.bfloat16)
    mixed = jnp.moveaxis(lax.map(one_channel, (jnp.moveaxis(left, -1, 0), jnp.moveaxis(right, -1, 0))), 0, -1)
    mixed = lax.optimization_barrier(mixed)
    return finish_pair(mixed, ready, mid_gain, out_weight, out_gate)
```

```python
import functools

import jax
import jax.numpy as jnp
from jax import lax
from jax.experimental import pallas as pl
from jax.experimental.pallas import tpu as pltpu
from jax.sharding import PartitionSpec as P

MESH = pl.DeviceIdType.MESH
NX, NY, NS = 4, 4, 16
BLK = 48
SUB = 16
NP = BLK // SUB
W = 128
KALL = BLK * NS
HALF_L = KALL // 2
HALF_R = W // 2


def unit_channels(values, channel_gain):
    centred = values - jnp.mean(values, axis=-1, keepdims=True)
    return (
        centred
        * lax.rsqrt(jnp.mean(centred * centred, axis=-1, keepdims=True) + 1e-05)
        * channel_gain
    )


def butterfly(slabs, first_stride):
    n = len(slabs)
    lane = lax.broadcasted_iota(jnp.int32, slabs[0].shape, 1)
    bit = 1
    while bit < n:
        stride = bit * first_stride
        low = (lane // stride) % 2 == 0
        out = list(slabs)
        for a in range(n):
            if a & bit:
                continue
            b = a | bit
            u, v = slabs[a], slabs[b]
            out[a] = jnp.where(low, u, pltpu.roll(v, stride, 1))
            out[b] = jnp.where(low, pltpu.roll(u, W - stride, 1), v)
        slabs = out
        bit *= 2
    return slabs


def kernel(
    x_ref, in_gain, left_w, right_w, mid_gain, out_w, out_gate,
    o_ref,
    ready, gate, send_l, send_r, land_r, left_g, right_g, stage, land_o,
    zs, zr, gs, gr, os_, or_,
):
    f, s = lax.axis_index("first"), lax.axis_index("second")
    y, x = f // NX, f % NX

    def dev(first, second):
        return {"first": first, "second": second}

    xp, xm = y * NX + (x + 1) % NX, y * NX + (x + NX - 1) % NX
    yp, ym = ((y + 1) % NY) * NX + x, ((y + NY - 1) % NY) * NX + x
    column = s % NX
    own = column == x

    barrier = pltpu.get_barrier_semaphore()

    def greet(first, second):
        pl.semaphore_signal(barrier, inc=1, device_id=dev(first, second), device_id_type=MESH)

    def greet_line(t, carry):
        greet(f, (s + t) % NS)
        return carry

    lax.fori_loop(1, NS, greet_line, 0)
    for peer in (xp, xm, yp, ym):
        greet(peer, s)

    def greet_senders(t, carry):
        first = y * NX + column

        @pl.when(jnp.logical_or(first != f, t != s))
        def _():
            greet(first, t)

        return carry

    lax.fori_loop(0, NS, greet_senders, 0)

    rows = lax.broadcasted_iota(jnp.int32, (W, W), 0)
    cols = lax.broadcasted_iota(jnp.int32, (W, W), 1)
    swap = (rows == (cols % 16) * 8 + cols // 16).astype(jnp.bfloat16)
    right_mix = jnp.dot(
        right_w[...], swap, preferred_element_type=jnp.float32
    ).astype(jnp.bfloat16)

    def line_copy(t, p, which):
        h = (t // 2 + 1) // 2 * (2 * ((t // 2) % 2) - 1)
        to = ((s // 2 + h + 8) % 8) * 2 + (s + t) % 2
        if which == 0:
            src, dst = send_l.at[to, p], left_g.at[p, x, pl.ds(pl.multiple_of(s * BLK, BLK), BLK)]
        else:
            src, dst = send_r.at[to, p], land_r.at[p, pl.ds(pl.multiple_of(s * BLK, BLK), BLK)]
        return pltpu.make_async_remote_copy(
            src_ref=src, dst_ref=dst, send_sem=zs.at[p, which], recv_sem=zr.at[p, which],
            device_id=dev(f, to), device_id_type=MESH,
        )

    def line_local(p, which):
        if which == 0:
            src, dst = send_l.at[s, p], left_g.at[p, x, pl.ds(pl.multiple_of(s * BLK, BLK), BLK)]
        else:
            src, dst = send_r.at[s, p], land_r.at[p, pl.ds(pl.multiple_of(s * BLK, BLK), BLK)]
        return pltpu.make_async_copy(src, dst, zr.at[p, which])

    def factor_piece(p):
        at = pl.multiple_of(p * SUB, SUB)
        values = x_ref[pl.ds(at, SUB)].reshape(SUB * BLK, W).astype(jnp.float32)
        r = unit_channels(values, in_gain[...]).astype(jnp.bfloat16)
        ready[pl.ds(at, SUB)] = r.reshape(SUB, BLK, W)
        for which, weight, stride, buf in ((0, left_w[...], 8, send_l), (1, right_mix, 1, send_r)):
            full = jnp.dot(r, weight, preferred_element_type=jnp.float32)
            full = full.astype(jnp.bfloat16).reshape(SUB, BLK, W)
            slabs = butterfly([full[i] for i in range(SUB)], stride)
            for i in range(SUB):
                buf[i, p] = slabs[i]

    def send_piece(p):
        for which in (0, 1):
            line_local(p, which).start()

            def go(t, carry, which=which):
                line_copy(t, p, which).start()
                return carry

            lax.fori_loop(1, NS, go, 0)

    factor_piece(0)
    pl.semaphore_wait(barrier, (NS - 1) + 4 + NS - own.astype(jnp.int32))

    def piece(p, carry):
        @pl.when(p > 0)
        def _():
            factor_piece(p)

        send_piece(p)
        return carry

    lax.fori_loop(0, NP, piece, 0)

    def gate_rows(i, carry):
        at = pl.multiple_of(i * SUB, SUB)
        r = ready[pl.ds(at, SUB)].reshape(SUB * BLK, W)
        g = jax.nn.sigmoid(jnp.dot(r, out_gate[...], preferred_element_type=jnp.float32))
        gate[pl.ds(at, SUB)] = g.reshape(SUB, BLK, W)
        return carry

    lax.fori_loop(0, NP, gate_rows, 0)

    def gather_copy(p, which, k):
        n = NX if which == 0 else NY
        at = x if which == 0 else y
        buf = left_g if which == 0 else right_g
        half = HALF_L if which == 0 else HALF_R
        up, down = (xp, xm) if which == 0 else (yp, ym)
        if k == 0 or k == 1:
            ref = buf.at[p, at]
        elif k == 2:
            ref = buf.at[p, (at + n - 1) % n, pl.ds(0, half)]
        else:
            ref = buf.at[p, (at + 1) % n, pl.ds(half, half)]
        return pltpu.make_async_remote_copy(
            src_ref=ref, dst_ref=ref, send_sem=gs.at[p, which, k], recv_sem=gr.at[p, which, k],
            device_id=dev(up if k % 2 == 0 else down, s), device_id_type=MESH,
        )

    def line_arrived(p, which):
        ref = left_g.at[p, x] if which == 0 else land_r.at[p]
        pltpu.make_async_copy(ref, ref, zr.at[p, which]).wait()

    def gather_first(p):
        line_arrived(p, 0)
        for k in (0, 1):
            gather_copy(p, 0, k).start()
        line_arrived(p, 1)
        right_g[p, y] = jnp.transpose(land_r[p])
        for k in (0, 1):
            gather_copy(p, 1, k).start()

    def gather_second(p):
        for which in (0, 1):
            for k in (0, 1):
                gather_copy(p, which, k).wait_recv()
                gather_copy(p, which, k + 2).start()

    def gather_last(p):
        for which in (0, 1):
            for k in (2, 3):
                gather_copy(p, which, k).wait_recv()

    lane_channel = lax.broadcasted_iota(jnp.int32, (SUB, W), 1) % 8

    def product(a, b):
        def one(v, carry):
            right = right_g[b, v]
            for h in range(2):
                left = jnp.concatenate([left_g[a, 2 * h], left_g[a, 2 * h + 1]], axis=1)
                full = jnp.dot(right, left, preferred_element_type=jnp.float32)
                for u in range(2):
                    tile = full[:, u * W : (u + 1) * W]
                    res = tile[:SUB]
                    for d in range(1, 8):
                        res = jnp.where(lane_channel == d, tile[d * SUB : (d + 1) * SUB], res)
                    res = (res * KALL ** (-0.5)).astype(jnp.bfloat16)
                    stage[(2 * h + u) * NY + v, a, pl.ds(pl.multiple_of(b * SUB, SUB), SUB)] = res
            return carry

        lax.fori_loop(0, NY, one, 0)

    runs = ((0, 0, 1), (0, 1, 1), (1, 0, 2), (0, 2, 1), (1, 2, 1), (2, 0, 3))

    def send_run(n):
        a, b, count = runs[n]
        sl = pl.ds(b * SUB, count * SUB)

        def go(t, carry):
            u, v = t // NY, t % NY
            u, v = (x + u) % NX, (s // NX + v) % NY
            first, second = y * NX + u, v * NX + x
            src, dst = stage.at[u * NY + v, a, sl], land_o.at[s, a, sl]
            mine = jnp.logical_and(first == f, second == s)

            @pl.when(mine)
            def _():
                pltpu.make_async_copy(src, dst, or_.at[n]).start()

            @pl.when(jnp.logical_not(mine))
            def _():
                pltpu.make_async_remote_copy(
                    src_ref=src, dst_ref=dst, send_sem=os_.at[n], recv_sem=or_.at[n],
                    device_id=dev(first, second), device_id_type=MESH,
                ).start()

            return carry

        lax.fori_loop(0, NX * NY, go, 0)

    def run_arrived(n):
        a, b, count = runs[n]
        ref = land_o.at[:, a, pl.ds(b * SUB, count * SUB)]
        pltpu.make_async_copy(ref, ref, or_.at[n]).wait()

    def finish(a, b):
        at = pl.ds(pl.multiple_of(b * SUB, SUB), SUB)
        slabs = butterfly([land_o[i, a, at] for i in range(NS)], 8)
        mixed = jnp.concatenate(slabs, axis=0).astype(jnp.float32)
        scaled = unit_channels(mixed, mid_gain[...]).astype(jnp.bfloat16)
        res = jnp.dot(scaled, out_w[...], preferred_element_type=jnp.float32)
        rows_ = pl.ds(pl.multiple_of(a * SUB, SUB), SUB)
        o_ref[rows_, at] = (res.reshape(SUB, SUB, W) * gate[rows_, at]).astype(jnp.bfloat16)

    gather_first(0)
    gather_second(0)
    gather_first(1)
    gather_last(0)
    product(0, 0)
    send_run(0)
    gather_second(1)
    gather_first(2)
    gather_last(1)
    product(0, 1)
    send_run(1)

    def more(b, carry):
        product(1, b)
        return carry

    lax.fori_loop(0, 2, more, 0)
    send_run(2)
    gather_second(2)
    gather_last(2)
    product(0, 2)
    send_run(3)
    product(1, 2)
    send_run(4)

    def most(b, carry):
        product(2, b)
        return carry

    lax.fori_loop(0, 3, most, 0)
    send_run(5)

    for n in range(6):
        run_arrived(n)
        a, b, count = runs[n]

        def fin(i, carry, a=a, b=b):
            finish(a, b + i)
            return carry

        lax.fori_loop(0, count, fin, 0)

    for p in range(NP):
        for which in (0, 1):
            buf = (send_l, send_r)[which]
            ref = buf.at[pl.ds(0, NS - 1), p]
            pltpu.make_async_copy(ref, ref, zs.at[p, which]).wait()
            for k in range(4):
                gather_copy(p, which, k).wait_send()
    for n in range(6):
        a, b, count = runs[n]
        sl = pl.ds(b * SUB, count * SUB)

        @pl.when(own)
        def _(n=n, a=a, sl=sl):
            ref = stage.at[pl.ds(0, NX * NY - 1), a, sl]
            pltpu.make_async_copy(ref, ref, os_.at[n]).wait()

        @pl.when(jnp.logical_not(own))
        def _(n=n, a=a, sl=sl):
            ref = stage.at[:, a, sl]
            pltpu.make_async_copy(ref, ref, os_.at[n]).wait()


def per_device(pair_state, in_gain, left_weight, right_weight, mid_gain, out_weight, out_gate):
    bf = jnp.bfloat16
    vmem = pl.BlockSpec(memory_space=pltpu.VMEM)
    return pl.pallas_call(
        kernel,
        out_shape=jax.ShapeDtypeStruct((BLK, BLK, W), bf),
        in_specs=[vmem] * 7,
        out_specs=vmem,
        scratch_shapes=[
            pltpu.VMEM((BLK, BLK, W), bf),
            pltpu.VMEM((BLK, BLK, W), jnp.float32),
            pltpu.VMEM((NS, NP, BLK, W), bf),
            pltpu.VMEM((NS, NP, BLK, W), bf),
            pltpu.VMEM((NP, KALL, W), bf),
            pltpu.VMEM((NP, NX, KALL, W), bf),
            pltpu.VMEM((NP, NY, W, KALL), bf),
            pltpu.VMEM((NX * NY, NP, BLK, W), bf),
            pltpu.VMEM((NS, NP, BLK, W), bf),
            pltpu.SemaphoreType.DMA((NP, 2)),
            pltpu.SemaphoreType.DMA((NP, 2)),
            pltpu.SemaphoreType.DMA((NP, 2, 4)),
            pltpu.SemaphoreType.DMA((NP, 2, 4)),
            pltpu.SemaphoreType.DMA((6,)),
            pltpu.SemaphoreType.DMA((6,)),
        ],
        compiler_params=pltpu.CompilerParams(
            collective_id=0, has_side_effects=True, vmem_limit_bytes=48 * 1024 * 1024
        ),
    )(pair_state, in_gain.reshape(1, W), left_weight, right_weight, mid_gain.reshape(1, W), out_weight, out_gate)


def solution(mesh):
    in_specs = (P("first", "second", None), P(), P(), P(), P(), P(), P())
    out_specs = P("first", "second", None)
    return jax.shard_map(
        per_device, mesh=mesh, in_specs=in_specs, out_specs=out_specs, check_vma=False
    )
```

```python
import functools

import jax
import jax.numpy as jnp
from jax import lax
from jax.experimental import pallas as pl
from jax.experimental.pallas import tpu as pltpu
from jax.sharding import PartitionSpec as P

MESH = pl.DeviceIdType.MESH
NX, NY, NS = 4, 4, 16
BLK = 48
SUB = 16
NP = BLK // SUB
W = 128
KALL = BLK * NS


def unit_channels(values, channel_gain):
    centred = values - jnp.mean(values, axis=-1, keepdims=True)
    return (
        centred
        * lax.rsqrt(jnp.mean(centred * centred, axis=-1, keepdims=True) + 1e-05)
        * channel_gain
    )


def butterfly(slabs, first_stride):
    n = len(slabs)
    lane = lax.broadcasted_iota(jnp.int32, slabs[0].shape, 1)
    bit = 1
    while bit < n:
        stride = bit * first_stride
        low = (lane // stride) % 2 == 0
        out = list(slabs)
        for a in range(n):
            if a & bit:
                continue
            b = a | bit
            u, v = slabs[a], slabs[b]
            out[a] = jnp.where(low, u, pltpu.roll(v, stride, 1))
            out[b] = jnp.where(low, pltpu.roll(u, W - stride, 1), v)
        slabs = out
        bit *= 2
    return slabs


def kernel(
    x_hbm, in_gain_hbm, left_hbm, right_hbm, mid_gain_hbm, out_hbm, gate_hbm,
    o_ref,
    x_ref, in_gain, left_w, right_w, mid_gain, out_w, out_gate, ls,
    ready, gate, send_l, send_r, land_r, left_g, right_g, stage, middle, land_o,
    zs, zr, gs, gr, hs, hr, os_, or_,
):
    f, s = lax.axis_index("first"), lax.axis_index("second")
    y, x = f // NX, f % NX

    def dev(first, second):
        return {"first": first, "second": second}

    turned = s % 2

    def pick(straight, crossed):
        return straight + turned * (crossed - straight)

    slot = (pick(x, y), pick(y, x))

    def ring(which, step):
        along_x, along_y = y * NX + (x + step) % NX, (y + step) % NY * NX + x
        return pick(along_x, along_y) if which == 0 else pick(along_y, along_x)


    loads = [
        pltpu.make_async_copy(src, dst, ls.at[n])
        for n, (src, dst) in enumerate((
            (right_hbm, right_w), (in_gain_hbm, in_gain), (left_hbm, left_w),
            (x_hbm.at[pl.ds(0, SUB)], x_ref.at[pl.ds(0, SUB)]),
            (x_hbm.at[pl.ds(SUB, BLK - SUB)], x_ref.at[pl.ds(SUB, BLK - SUB)]),
            (gate_hbm, out_gate), (mid_gain_hbm, mid_gain), (out_hbm, out_w),
        ))
    ]
    for load in loads:
        load.start()

    barrier = pltpu.get_barrier_semaphore()

    def greet(first, second):
        pl.semaphore_signal(barrier, inc=1, device_id=dev(first, second), device_id_type=MESH)

    def greet_line(t, carry):
        greet(f, (s + t) % NS)
        return carry

    lax.fori_loop(1, NS, greet_line, 0)
    for step in (1, NX - 1):
        for which in (0, 1):
            greet(ring(which, step), s)
    greet(ring(0, 2), s)


    rows = lax.broadcasted_iota(jnp.int32, (W, W), 0)
    cols = lax.broadcasted_iota(jnp.int32, (W, W), 1)
    swap = (rows == (cols % 16) * 8 + cols // 16).astype(jnp.bfloat16)
    loads[0].wait()
    right_mix = jnp.dot(
        right_w[...], swap, preferred_element_type=jnp.float32
    ).astype(jnp.bfloat16)

    def line_copy(t, p, which):
        h = (t // 2 + 1) // 2 * (2 * ((t // 2) % 2) - 1)
        to = ((s // 2 + h + 8) % 8) * 2 + (s + t) % 2
        if which == 0:
            there = x + to % 2 * (y - x)
            src, dst = send_l.at[to, p], left_g.at[p, there, pl.ds(pl.multiple_of(s * BLK, BLK), BLK)]
        else:
            src, dst = send_r.at[to, p], land_r.at[p, pl.ds(pl.multiple_of(s * BLK, BLK), BLK)]
        return pltpu.make_async_remote_copy(
            src_ref=src, dst_ref=dst, send_sem=zs.at[p, which], recv_sem=zr.at[p, which],
            device_id=dev(f, to), device_id_type=MESH,
        )

    def line_local(p, which):
        if which == 0:
            src, dst = send_l.at[s, p], left_g.at[p, slot[0], pl.ds(pl.multiple_of(s * BLK, BLK), BLK)]
        else:
            src, dst = send_r.at[s, p], land_r.at[p, pl.ds(pl.multiple_of(s * BLK, BLK), BLK)]
        return pltpu.make_async_copy(src, dst, zr.at[p, which])

    def factor_piece(p):
        at = pl.multiple_of(p * SUB, SUB)
        values = x_ref[pl.ds(at, SUB)].reshape(SUB * BLK, W).astype(jnp.float32)
        r = unit_channels(values, in_gain[...]).astype(jnp.bfloat16)
        ready[pl.ds(at, SUB)] = r.reshape(SUB, BLK, W)
        for which, weight, stride, buf in ((0, left_w[...], 8, send_l), (1, right_mix, 1, send_r)):
            full = jnp.dot(r, weight, preferred_element_type=jnp.float32)
            full = full.astype(jnp.bfloat16).reshape(SUB, BLK, W)
            slabs = butterfly([full[i] for i in range(SUB)], stride)
            for i in range(SUB):
                buf[i, p] = slabs[i]

    def send_piece(which, p):
        line_local(p, which).start()

        def go(t, carry):
            line_copy(t, p, which).start()
            return carry

        lax.fori_loop(1, NS, go, 0)

    def gate_rows(i, carry):
        at = pl.multiple_of(i * SUB, SUB)
        r = ready[pl.ds(at, SUB)].reshape(SUB * BLK, W)
        g = jax.nn.sigmoid(jnp.dot(r, out_gate[...], preferred_element_type=jnp.float32))
        gate[pl.ds(at, SUB)] = g.reshape(SUB, BLK, W)
        return carry

    def piece(p, carry):
        factor_piece(p)
        return carry

    for load in loads[1:]:
        load.wait()
    with jax.named_scope("factor"):
        lax.fori_loop(0, NP, piece, 0)
    with jax.named_scope("gate"):
        lax.fori_loop(0, NP, gate_rows, 0)
    with jax.named_scope("barrier"):
        pl.semaphore_wait(barrier, (NS - 1) + 5)
    with jax.named_scope("send"):
        for p in range(NP):
            for which in (0, 1):
                send_piece(which, p)

    def ring_copy(which, p, block, part, step, sem):
        buf = (left_g, right_g)[which]
        size = buf.shape[2] // 2
        ref = buf.at[p, block, pl.ds(part * size, size)]
        return pltpu.make_async_remote_copy(
            src_ref=ref, dst_ref=ref, send_sem=gs.at[p, which], recv_sem=gr.at[p, which, sem],
            device_id=dev(ring(which, step), s), device_id_type=MESH,
        )

    def ring_wait(which, p, blocks, part, sem):
        buf = (left_g, right_g)[which]
        size = buf.shape[2] // 2
        ref = buf.at[p, pl.ds(0, blocks), pl.ds(part * size, size)]
        if blocks > 1:
            ref = buf.at[p, pl.ds(0, blocks)]
        pltpu.make_async_copy(ref, ref, sem).wait()

    def gather(which, p):
        with jax.named_scope(f"line{which}{p}"):
            ref = left_g.at[p, slot[0]] if which == 0 else land_r.at[p]
            pltpu.make_async_copy(ref, ref, zr.at[p, which]).wait()
        if which == 1:
            with jax.named_scope(f"turn{p}"):
                right_g[p, slot[1]] = jnp.transpose(land_r[p])
        me = slot[which]
        ring_copy(which, p, me, 0, 1, 0).start()
        ring_copy(which, p, me, 1, NX - 1, 1).start()
        ring_copy(which, p, me, 1, 1, 2).start()
        ring_copy(which, p, me, 0, NX - 1, 2).start()

    def pass_on(which, p):
        with jax.named_scope(f"pass{which}{p}"):
            ring_wait(which, p, 1, 0, gr.at[p, which, 0])
            ring_copy(which, p, (slot[which] + NX - 1) % NX, 0, 1, 2).start()
            ring_wait(which, p, 1, 1, gr.at[p, which, 1])
            ring_copy(which, p, (slot[which] + 1) % NX, 1, NX - 1, 2).start()

    def gathered(which, p):
        with jax.named_scope(f"gathered{which}{p}"):
            ring_wait(which, p, 2, 0, gr.at[p, which, 2])

    lane_channel = lax.broadcasted_iota(jnp.int32, (SUB, W), 1) % 8

    def product(a, b):
        with jax.named_scope(f"prod{a}{b}"):
            right = right_g[b].reshape(NY * W, KALL)
            for h in range(2):
                left = jnp.concatenate([left_g[a, 2 * h], left_g[a, 2 * h + 1]], axis=1)
                full = jnp.dot(right, left, preferred_element_type=jnp.float32)
                for v in range(NY):
                    for u in range(2):
                        tile = full[v * W : (v + 1) * W, u * W : (u + 1) * W]
                        res = tile[:SUB]
                        for d in range(1, 8):
                            res = jnp.where(lane_channel == d, tile[d * SUB : (d + 1) * SUB], res)
                        res = (res * KALL ** (-0.5)).astype(jnp.bfloat16)
                        stage[2 * h + u, b, a, v] = res

    def hop_copy(a, b, step):
        to = (slot[0] + step) % NX
        return pltpu.make_async_remote_copy(
            src_ref=stage.at[to, b, a], dst_ref=middle.at[slot[0], b, a],
            send_sem=hs.at[b, a], recv_sem=hr.at[b, a],
            device_id=dev(ring(0, step), s), device_id_type=MESH,
        )

    def hop(a, b):
        for step in (2, 1, 3):
            hop_copy(a, b, step).start()
        middle[slot[0], b, a] = stage[slot[0], b, a]

    def spread(a, b):
        with jax.named_scope(f"hopwait{a}{b}"):
            ref = middle.at[pl.ds(0, 3), b, a]
            pltpu.make_async_copy(ref, ref, hr.at[b, a]).wait()

        def source(to):
            w, v = pick(to % NX, to // NX), pick(to // NX, to % NX)
            return middle.at[w, b, a, v]

        def go(t, carry):
            h = (t // 2 + 1) // 2 * (2 * ((t // 2) % 2) - 1)
            to = ((s // 2 + h + 8) % 8) * 2 + (s + t) % 2
            pltpu.make_async_remote_copy(
                src_ref=source(to), dst_ref=land_o.at[s, b, a],
                send_sem=os_.at[b, a], recv_sem=or_.at[b, a],
                device_id=dev(f, to), device_id_type=MESH,
            ).start()
            return carry

        with jax.named_scope(f"spread{a}{b}"):
            lax.fori_loop(1, NS, go, 0)
            pltpu.make_async_copy(source(s), land_o.at[s, b, a], or_.at[b, a]).start()

    def arrived(a, b):
        ref = land_o.at[:, b, a]
        with jax.named_scope(f"arrive{a}{b}"):
            pltpu.make_async_copy(ref, ref, or_.at[b, a]).wait()

    def finish(a, b):
        with jax.named_scope(f"fin{a}{b}"):
            at = pl.ds(b * SUB, SUB)
            rows_ = pl.ds(a * SUB, SUB)
            slabs = butterfly([land_o[i, b, a] for i in range(NS)], 8)
            mixed = jnp.concatenate(slabs, axis=0).astype(jnp.float32)
            scaled = unit_channels(mixed, mid_gain[...]).astype(jnp.bfloat16)
            res = jnp.dot(scaled, out_w[...], preferred_element_type=jnp.float32)
            o_ref[rows_, at] = (res.reshape(SUB, SUB, W) * gate[rows_, at]).astype(jnp.bfloat16)

    def make(a, b):
        product(a, b)
        hop(a, b)

    def end(a, b):
        arrived(a, b)
        finish(a, b)

    left, right = 0, 1
    gather(left, 0)
    gather(right, 0)
    pass_on(left, 0)
    gather(left, 1)
    pass_on(right, 0)
    gathered(left, 0)
    gather(right, 1)
    pass_on(left, 1)
    gathered(right, 0)
    make(0, 0)
    gather(left, 2)
    pass_on(right, 1)
    gathered(left, 1)
    make(1, 0)
    gather(right, 2)
    spread(0, 0)
    pass_on(left, 2)
    gathered(right, 1)
    make(0, 1)
    pass_on(right, 2)
    make(1, 1)
    spread(1, 0)
    gathered(left, 2)
    make(2, 0)
    spread(0, 1)
    make(2, 1)
    spread(1, 1)
    gathered(right, 2)
    make(0, 2)
    spread(2, 0)
    make(1, 2)
    spread(2, 1)
    make(2, 2)
    end(0, 0)
    spread(0, 2)
    end(1, 0)
    spread(1, 2)
    spread(2, 2)
    end(0, 1)
    end(1, 1)
    end(2, 0)
    end(2, 1)
    end(0, 2)
    end(1, 2)
    end(2, 2)

    for p in range(NP):
        for which in (0, 1):
            buf = (send_l, send_r)[which]
            ref = buf.at[pl.ds(0, NS - 1), p]
            pltpu.make_async_copy(ref, ref, zs.at[p, which]).wait()
            ring_wait(which, p, 3, 0, gs.at[p, which])
    for b in range(NP):
        for a in range(NP):
            ref = middle.at[pl.ds(0, 3), b, a]
            pltpu.make_async_copy(ref, ref, hs.at[b, a]).wait()
            ref = land_o.at[pl.ds(0, NS - 1), b, a]
            pltpu.make_async_copy(ref, ref, os_.at[b, a]).wait()


def per_device(pair_state, in_gain, left_weight, right_weight, mid_gain, out_weight, out_gate):
    bf = jnp.bfloat16
    vmem = pl.BlockSpec(memory_space=pltpu.VMEM)
    return pl.pallas_call(
        kernel,
        out_shape=jax.ShapeDtypeStruct((BLK, BLK, W), bf),
        in_specs=[pl.BlockSpec(memory_space=pltpu.HBM)] * 7,
        out_specs=vmem,
        scratch_shapes=[
            pltpu.VMEM((BLK, BLK, W), bf),
            pltpu.VMEM((1, W), jnp.float32),
            pltpu.VMEM((W, W), bf),
            pltpu.VMEM((W, W), bf),
            pltpu.VMEM((1, W), jnp.float32),
            pltpu.VMEM((W, W), bf),
            pltpu.VMEM((W, W), bf),
            pltpu.SemaphoreType.DMA((8,)),
            pltpu.VMEM((BLK, BLK, W), bf),
            pltpu.VMEM((BLK, BLK, W), jnp.float32),
            pltpu.VMEM((NS, NP, BLK, W), bf),
            pltpu.VMEM((NS, NP, BLK, W), bf),
            pltpu.VMEM((NP, KALL, W), bf),
            pltpu.VMEM((NP, NX, KALL, W), bf),
            pltpu.VMEM((NP, NY, W, KALL), bf),
            pltpu.VMEM((NX, NP, NP, NY, SUB, W), bf),
            pltpu.VMEM((NX, NP, NP, NY, SUB, W), bf),
            pltpu.VMEM((NS, NP, NP, SUB, W), bf),
            pltpu.SemaphoreType.DMA((NP, 2)),
            pltpu.SemaphoreType.DMA((NP, 2)),
            pltpu.SemaphoreType.DMA((NP, 2)),
            pltpu.SemaphoreType.DMA((NP, 2, 3)),
            pltpu.SemaphoreType.DMA((NP, NP)),
            pltpu.SemaphoreType.DMA((NP, NP)),
            pltpu.SemaphoreType.DMA((NP, NP)),
            pltpu.SemaphoreType.DMA((NP, NP)),
        ],
        compiler_params=pltpu.CompilerParams(
            collective_id=0, has_side_effects=True, vmem_limit_bytes=50_331_648
        ),
    )(*(pltpu.with_memory_space_constraint(v, pltpu.HBM) for v in (pair_state, in_gain.reshape(1, W), left_weight, right_weight, mid_gain.reshape(1, W), out_weight, out_gate)))


def solution(mesh):
    in_specs = (P("first", "second", None), P(), P(), P(), P(), P(), P())
    out_specs = P("first", "second", None)
    return jax.shard_map(
        per_device, mesh=mesh, in_specs=in_specs, out_specs=out_specs, check_vma=False
    )
```

```python
import functools

import jax
import jax.numpy as jnp
from jax import lax
from jax.experimental import pallas as pl
from jax.experimental.pallas import tpu as pltpu
from jax.sharding import PartitionSpec as P

MESH = pl.DeviceIdType.MESH
NX, NY, NS = 4, 4, 16
BLK = 48
SUB = 16
NP = BLK // SUB
W = 128
KALL = BLK * NS
NQ = BLK // SUB
PART = NS * SUB
UNITS = (
    (0, 0, 0, 3),
    (1, 0, 0, 3),
    (0, 1, 0, 3),
    (1, 1, 0, 3),
    (0, 2, 0, 3),
    (1, 2, 0, 2),
    (1, 2, 2, 3),
)


PEERS = tuple((h, other) for other in (0, 1) for h in (4, 3, -3, 2, -2, 1, -1, 0) if (h, other) != (0, 0))


def unit_channels(values, channel_gain):
    centred = values - jnp.mean(values, axis=-1, keepdims=True)
    return (
        centred
        * lax.rsqrt(jnp.mean(centred * centred, axis=-1, keepdims=True) + 1e-05)
        * channel_gain
    )


def butterfly(slabs, first_stride):
    n = len(slabs)
    lane = lax.broadcasted_iota(jnp.int32, slabs[0].shape, 1)
    bit = 1
    while bit < n:
        stride = bit * first_stride
        low = (lane // stride) % 2 == 0
        out = list(slabs)
        for a in range(n):
            if a & bit:
                continue
            b = a | bit
            u, v = slabs[a], slabs[b]
            out[a] = jnp.where(low, u, pltpu.roll(v, stride, 1))
            out[b] = jnp.where(low, pltpu.roll(u, W - stride, 1), v)
        slabs = out
        bit *= 2
    return slabs


def kernel(
    x_hbm, in_gain_hbm, left_hbm, right_hbm, mid_gain_hbm, out_hbm, gate_hbm,
    o_ref,
    x_ref, in_gain, left_w, right_w, mid_gain, out_w, out_gate, ls,
    ready, gate, send_l, send_r, land_r, left_g, right_g, stage, middle, land_o,
    zs, zr, gs, gr, hs, hr, os_, or_,
):
    f, s = lax.axis_index("first"), lax.axis_index("second")
    y, x = f // NX, f % NX

    def dev(first, second):
        return {"first": first, "second": second}

    turned = s % 2

    def pick(straight, crossed):
        return straight + turned * (crossed - straight)

    slot = (pick(x, y), pick(y, x))

    def ring(which, step):
        along_x, along_y = y * NX + (x + step) % NX, (y + step) % NY * NX + x
        return pick(along_x, along_y) if which == 0 else pick(along_y, along_x)


    loads = [
        pltpu.make_async_copy(src, dst, ls.at[n])
        for n, (src, dst) in enumerate((
            (right_hbm, right_w), (in_gain_hbm, in_gain), (left_hbm, left_w),
            (x_hbm.at[pl.ds(0, SUB)], x_ref.at[pl.ds(0, SUB)]),
            (x_hbm.at[pl.ds(SUB, BLK - SUB)], x_ref.at[pl.ds(SUB, BLK - SUB)]),
            (gate_hbm, out_gate), (mid_gain_hbm, mid_gain), (out_hbm, out_w),
        ))
    ]
    for load in loads:
        load.start()

    barrier = pltpu.get_barrier_semaphore()

    def greet(first, second):
        pl.semaphore_signal(barrier, inc=1, device_id=dev(first, second), device_id_type=MESH)

    def greet_line(t, carry):
        greet(f, (s + t) % NS)
        return carry

    lax.fori_loop(1, NS, greet_line, 0)
    for step in (1, NX - 1):
        for which in (0, 1):
            greet(ring(which, step), s)
    greet(ring(0, 2), s)


    rows = lax.broadcasted_iota(jnp.int32, (W, W), 0)
    cols = lax.broadcasted_iota(jnp.int32, (W, W), 1)
    swap = (rows == (cols % 16) * 8 + cols // 16).astype(jnp.bfloat16)
    loads[0].wait()
    right_mix = jnp.dot(
        right_w[...], swap, preferred_element_type=jnp.float32
    ).astype(jnp.bfloat16)

    def line_peer(t):
        h, other = PEERS[t]
        return ((s // 2 + h + 8) % 8) * 2 + (s + other) % 2

    def for_peers(go):
        for t in range(NS - 1):
            go(t, 0)

    rows_s = pl.ds(pl.multiple_of(s * SUB, SUB), SUB)

    def line_ends(n, to):
        which, p, q0, q1 = UNITS[n]
        parts = pl.ds(q0, q1 - q0)
        if which == 0:
            there = x + to % 2 * (y - x)
            return send_l.at[to, p, parts], left_g.at[p, there, parts, rows_s]
        return send_r.at[to, p, parts], land_r.at[p, parts, rows_s]

    def line_copy(n, t):
        to = line_peer(t)
        src, dst = line_ends(n, to)
        return pltpu.make_async_remote_copy(
            src_ref=src, dst_ref=dst, send_sem=zs.at[n], recv_sem=zr.at[n],
            device_id=dev(f, to), device_id_type=MESH,
        )

    def norm_piece(p):
        at = pl.ds(p * SUB, SUB)
        values = x_ref[at].reshape(SUB * BLK, W).astype(jnp.float32)
        ready[at] = unit_channels(values, in_gain[...]).astype(jnp.bfloat16).reshape(SUB, BLK, W)

    def factor_piece(which, p):
        r = ready[pl.ds(p * SUB, SUB)].reshape(SUB * BLK, W)
        weight, stride, buf = ((left_w[...], 8, send_l), (right_mix, 1, send_r))[which]
        full = jnp.dot(r, weight, preferred_element_type=jnp.float32)
        full = full.astype(jnp.bfloat16).reshape(SUB, BLK, W)
        slabs = butterfly([full[i] for i in range(SUB)], stride)
        for i in range(SUB):
            buf[i, p] = slabs[i].reshape(NQ, SUB, W)

    def send(n):
        src, dst = line_ends(n, s)
        pltpu.make_async_copy(src, dst, zr.at[n]).start()

        def go(t, carry):
            line_copy(n, t).start()
            return carry

        for_peers(go)

    def gate_rows(i, carry):
        at = pl.multiple_of(i * SUB, SUB)
        r = ready[pl.ds(at, SUB)].reshape(SUB * BLK, W)
        g = jax.nn.sigmoid(jnp.dot(r, out_gate[...], preferred_element_type=jnp.float32))
        gate[pl.ds(at, SUB)] = g.reshape(SUB, BLK, W)
        return carry

    loads[1].wait()
    loads[2].wait()
    loads[3].wait()
    with jax.named_scope("factor"):
        norm_piece(0)
        factor_piece(0, 0)
    with jax.named_scope("barrier"):
        pl.semaphore_wait(barrier, (NS - 1) + 5)
    with jax.named_scope("send"):
        done = {(0, 0)}
        for n, (which, p, q0, q1) in enumerate(UNITS):
            if (which, p) not in done:
                if (1 - which, p) not in done:
                    if p == 1:
                        loads[4].wait()
                    norm_piece(p)
                factor_piece(which, p)
                done.add((which, p))
            send(n)
    for load in loads[5:]:
        load.wait()
    with jax.named_scope("gate"):
        lax.fori_loop(0, NP, gate_rows, 0)

    def ring_part(n, blocks, half=None):
        which, p, q0, q1 = UNITS[n]
        parts = q1 - q0
        if which == 0:
            rows_ = pl.ds(0, PART) if half is None else pl.ds(half * (PART // 2), PART // 2)
            return left_g.at[p, blocks, pl.ds(q0, parts), rows_]
        rows_ = pl.ds(0, W) if half is None else pl.ds(half * (W // 2), W // 2)
        return right_g.at[p, blocks, rows_, pl.ds(q0 * PART, parts * PART)]

    def ring_copy(n, block, half, step, sem):
        ref = ring_part(n, block, half)
        return pltpu.make_async_remote_copy(
            src_ref=ref, dst_ref=ref, send_sem=gs.at[n], recv_sem=gr.at[n, sem],
            device_id=dev(ring(UNITS[n][0], step), s), device_id_type=MESH,
        )

    def wait_for(ref, sem):
        pltpu.make_async_copy(ref, ref, sem).wait()

    def gather(n):
        which, p, q0, q1 = UNITS[n]
        parts = pl.ds(q0, q1 - q0)
        with jax.named_scope(f"line{n}"):
            wait_for(left_g.at[p, slot[0], parts] if which == 0 else land_r.at[p, parts], zr.at[n])
        if which == 1:
            with jax.named_scope(f"turn{n}"):
                block = land_r[p, q0:q1].reshape((q1 - q0) * PART, W)
                right_g[p, slot[1], :, q0 * PART : q1 * PART] = jnp.transpose(block)
        me = slot[which]
        ring_copy(n, me, 0, 1, 0).start()
        ring_copy(n, me, 1, NX - 1, 1).start()
        ring_copy(n, me, 1, 1, 2).start()
        ring_copy(n, me, 0, NX - 1, 2).start()

    def pass_on(n):
        me = slot[UNITS[n][0]]
        with jax.named_scope(f"pass{n}"):
            wait_for(ring_part(n, 0, 0), gr.at[n, 0])
            ring_copy(n, (me + NX - 1) % NX, 0, 1, 2).start()
            wait_for(ring_part(n, 0, 1), gr.at[n, 1])
            ring_copy(n, (me + 1) % NX, 1, NX - 1, 2).start()

    def gathered(n):
        with jax.named_scope(f"gathered{n}"):
            wait_for(ring_part(n, pl.ds(0, 2)), gr.at[n, 2])

    lane_channel = lax.broadcasted_iota(jnp.int32, (SUB, W), 1) % 8

    def product(a, b):
        with jax.named_scope(f"prod{a}{b}"):
            right = right_g[b].reshape(NY * W, KALL)
            for h in range(2):
                left = jnp.concatenate(
                    [left_g[a, 2 * h + u].reshape(KALL, W) for u in range(2)], axis=1
                )
                full = jnp.dot(right, left, preferred_element_type=jnp.float32)
                for v in range(NY):
                    for u in range(2):
                        tile = full[v * W : (v + 1) * W, u * W : (u + 1) * W]
                        res = tile[:SUB]
                        for d in range(1, 8):
                            res = jnp.where(lane_channel == d, tile[d * SUB : (d + 1) * SUB], res)
                        res = (res * KALL ** (-0.5)).astype(jnp.bfloat16)
                        stage[2 * h + u, b, a, v] = res

    def hop_copy(a, b, step):
        to = (slot[0] + step) % NX
        return pltpu.make_async_remote_copy(
            src_ref=stage.at[to, b, a], dst_ref=middle.at[slot[0], b, a],
            send_sem=hs.at[b, a], recv_sem=hr.at[b, a],
            device_id=dev(ring(0, step), s), device_id_type=MESH,
        )

    def hop(a, b):
        for step in (2, 1, 3):
            hop_copy(a, b, step).start()
        middle[slot[0], b, a] = stage[slot[0], b, a]

    def spread(a, b):
        with jax.named_scope(f"hopwait{a}{b}"):
            ref = middle.at[pl.ds(0, 3), b, a]
            pltpu.make_async_copy(ref, ref, hr.at[b, a]).wait()

        def source(to):
            w, v = pick(to % NX, to // NX), pick(to // NX, to % NX)
            return middle.at[w, b, a, v]

        def go(t, carry):
            to = line_peer(t)
            pltpu.make_async_remote_copy(
                src_ref=source(to), dst_ref=land_o.at[s, b, a],
                send_sem=os_.at[b, a], recv_sem=or_.at[b, a],
                device_id=dev(f, to), device_id_type=MESH,
            ).start()
            return carry

        with jax.named_scope(f"spread{a}{b}"):
            for_peers(go)
            pltpu.make_async_copy(source(s), land_o.at[s, b, a], or_.at[b, a]).start()

    def arrived(a, b):
        ref = land_o.at[:, b, a]
        with jax.named_scope(f"arrive{a}{b}"):
            pltpu.make_async_copy(ref, ref, or_.at[b, a]).wait()

    def finish(a, b):
        with jax.named_scope(f"fin{a}{b}"):
            at = pl.ds(b * SUB, SUB)
            rows_ = pl.ds(a * SUB, SUB)
            slabs = butterfly([land_o[i, b, a] for i in range(NS)], 8)
            mixed = jnp.concatenate(slabs, axis=0).astype(jnp.float32)
            scaled = unit_channels(mixed, mid_gain[...]).astype(jnp.bfloat16)
            res = jnp.dot(scaled, out_w[...], preferred_element_type=jnp.float32)
            o_ref[rows_, at] = (res.reshape(SUB, SUB, W) * gate[rows_, at]).astype(jnp.bfloat16)

    def make(a, b):
        product(a, b)
        hop(a, b)

    def end(a, b):
        arrived(a, b)
        finish(a, b)

    def drain_tiles(tiles):
        for a, b in tiles:
            wait_for(middle.at[pl.ds(0, 3), b, a], hs.at[b, a])
            wait_for(land_o.at[pl.ds(0, NS - 1), b, a], os_.at[b, a])

    def drain():
        for n, (which, p, q0, q1) in enumerate(UNITS):
            wait_for((send_l, send_r)[which].at[pl.ds(0, NS - 1), p, pl.ds(q0, q1 - q0)], zs.at[n])
            wait_for(ring_part(n, pl.ds(0, 3)), gs.at[n])
        drain_tiles(((0, 0), (1, 0), (0, 1), (1, 1), (2, 0)))

    gather(0)
    gather(1)
    pass_on(0)
    gather(2)
    pass_on(1)
    gathered(0)
    gather(3)
    pass_on(2)
    gathered(1)
    make(0, 0)
    gather(4)
    pass_on(3)
    gathered(2)
    make(1, 0)
    gather(5)
    spread(0, 0)
    gather(6)
    pass_on(4)
    gathered(3)
    make(0, 1)
    pass_on(5)
    make(1, 1)
    spread(1, 0)
    pass_on(6)
    gathered(4)
    make(2, 0)
    spread(0, 1)
    make(2, 1)
    spread(1, 1)
    gathered(5)
    gathered(6)
    make(0, 2)
    make(1, 2)
    make(2, 2)
    spread(2, 0)
    spread(2, 1)
    spread(0, 2)
    end(0, 0)
    spread(1, 2)
    end(1, 0)
    spread(2, 2)
    end(0, 1)
    end(1, 1)
    end(2, 0)
    end(2, 1)
    drain()
    end(0, 2)
    end(1, 2)
    end(2, 2)

    drain_tiles(((2, 1), (0, 2), (1, 2), (2, 2)))


def per_device(pair_state, in_gain, left_weight, right_weight, mid_gain, out_weight, out_gate):
    bf = jnp.bfloat16
    vmem = pl.BlockSpec(memory_space=pltpu.VMEM)
    return pl.pallas_call(
        kernel,
        out_shape=jax.ShapeDtypeStruct((BLK, BLK, W), bf),
        in_specs=[pl.BlockSpec(memory_space=pltpu.HBM)] * 7,
        out_specs=vmem,
        scratch_shapes=[
            pltpu.VMEM((BLK, BLK, W), bf),
            pltpu.VMEM((1, W), jnp.float32),
            pltpu.VMEM((W, W), bf),
            pltpu.VMEM((W, W), bf),
            pltpu.VMEM((1, W), jnp.float32),
            pltpu.VMEM((W, W), bf),
            pltpu.VMEM((W, W), bf),
            pltpu.SemaphoreType.DMA((8,)),
            pltpu.VMEM((BLK, BLK, W), bf),
            pltpu.VMEM((BLK, BLK, W), jnp.float32),
            pltpu.VMEM((NS, NP, NQ, SUB, W), bf),
            pltpu.VMEM((NS, NP, NQ, SUB, W), bf),
            pltpu.VMEM((NP, NQ, PART, W), bf),
            pltpu.VMEM((NP, NX, NQ, PART, W), bf),
            pltpu.VMEM((NP, NY, W, KALL), bf),
            pltpu.VMEM((NX, NP, NP, NY, SUB, W), bf),
            pltpu.VMEM((NX, NP, NP, NY, SUB, W), bf),
            pltpu.VMEM((NS, NP, NP, SUB, W), bf),
            pltpu.SemaphoreType.DMA((len(UNITS),)),
            pltpu.SemaphoreType.DMA((len(UNITS),)),
            pltpu.SemaphoreType.DMA((len(UNITS),)),
            pltpu.SemaphoreType.DMA((len(UNITS), 3)),
            pltpu.SemaphoreType.DMA((NP, NP)),
            pltpu.SemaphoreType.DMA((NP, NP)),
            pltpu.SemaphoreType.DMA((NP, NP)),
            pltpu.SemaphoreType.DMA((NP, NP)),
        ],
        compiler_params=pltpu.CompilerParams(
            collective_id=0, has_side_effects=True, vmem_limit_bytes=50_331_648
        ),
    )(*(pltpu.with_memory_space_constraint(v, pltpu.HBM) for v in (pair_state, in_gain.reshape(1, W), left_weight, right_weight, mid_gain.reshape(1, W), out_weight, out_gate)))


def solution(mesh):
    in_specs = (P("first", "second", None), P(), P(), P(), P(), P(), P())
    out_specs = P("first", "second", None)
    return jax.shard_map(
        per_device, mesh=mesh, in_specs=in_specs, out_specs=out_specs, check_vma=False
    )
```

```python
import functools

import jax
import jax.numpy as jnp
from jax import lax
from jax.experimental import pallas as pl
from jax.experimental.pallas import tpu as pltpu
from jax.sharding import PartitionSpec as P

MESH = pl.DeviceIdType.MESH
NX, NY, NS = 4, 4, 16
BLK = 48
SUB = 16
NP = BLK // SUB
W = 128
KALL = BLK * NS
NQ = BLK // SUB
PART = NS * SUB
UNITS = (
    (0, 0, 0, 3),
    (1, 0, 0, 3),
    (0, 1, 0, 3),
    (1, 1, 0, 3),
    (0, 2, 0, 3),
    (1, 2, 0, 2),
    (1, 2, 2, 3),
)


PEERS = tuple((h, other) for other in (0, 1) for h in (4, 3, -3, 2, -2, 1, -1, 0) if (h, other) != (0, 0))


AHEAD = (2, 1, 3)


def unit_channels(values, channel_gain):
    centred = values - jnp.mean(values, axis=-1, keepdims=True)
    return (
        centred
        * lax.rsqrt(jnp.mean(centred * centred, axis=-1, keepdims=True) + 1e-05)
        * channel_gain
    )


def butterfly(slabs, first_stride):
    n = len(slabs)
    lane = lax.broadcasted_iota(jnp.int32, slabs[0].shape, 1)
    bit = 1
    while bit < n:
        stride = bit * first_stride
        low = (lane // stride) % 2 == 0
        out = list(slabs)
        for a in range(n):
            if a & bit:
                continue
            b = a | bit
            u, v = slabs[a], slabs[b]
            out[a] = jnp.where(low, u, pltpu.roll(v, stride, 1))
            out[b] = jnp.where(low, pltpu.roll(u, W - stride, 1), v)
        slabs = out
        bit *= 2
    return slabs


def kernel(
    x_hbm, in_gain_hbm, left_hbm, right_hbm, mid_gain_hbm, out_hbm, gate_hbm,
    o_ref,
    x_ref, in_gain, left_w, right_w, mid_gain, out_w, out_gate, ls,
    ready, gate, send_l, send_r, land_r, left_g, right_g, stage, middle, land_o,
    zs, zr, gs, gr, hs, hr, os_, or_,
):
    f, s = lax.axis_index("first"), lax.axis_index("second")
    y, x = f // NX, f % NX

    def dev(first, second):
        return {"first": first, "second": second}

    turned = s % 2

    def pick(straight, crossed):
        return straight + turned * (crossed - straight)

    slot = (pick(x, y), pick(y, x))

    def ring(which, step):
        along_x, along_y = y * NX + (x + step) % NX, (y + step) % NY * NX + x
        return pick(along_x, along_y) if which == 0 else pick(along_y, along_x)


    loads = [
        pltpu.make_async_copy(src, dst, ls.at[n])
        for n, (src, dst) in enumerate((
            (right_hbm, right_w), (in_gain_hbm, in_gain), (left_hbm, left_w),
            (x_hbm.at[pl.ds(0, SUB)], x_ref.at[pl.ds(0, SUB)]),
            (x_hbm.at[pl.ds(SUB, BLK - SUB)], x_ref.at[pl.ds(SUB, BLK - SUB)]),
            (gate_hbm, out_gate), (mid_gain_hbm, mid_gain), (out_hbm, out_w),
        ))
    ]
    for load in loads:
        load.start()

    barrier = pltpu.get_barrier_semaphore()

    def greet(first, second):
        pl.semaphore_signal(barrier, inc=1, device_id=dev(first, second), device_id_type=MESH)

    def greet_line(t, carry):
        greet(f, (s + t) % NS)
        return carry

    lax.fori_loop(1, NS, greet_line, 0)
    for step in (1, NX - 1):
        for which in (0, 1):
            greet(ring(which, step), s)
    greet(ring(0, 2), s)


    rows = lax.broadcasted_iota(jnp.int32, (W, W), 0)
    cols = lax.broadcasted_iota(jnp.int32, (W, W), 1)
    swap = (rows == (cols % 16) * 8 + cols // 16).astype(jnp.bfloat16)
    loads[0].wait()
    right_mix = jnp.dot(
        right_w[...], swap, preferred_element_type=jnp.float32
    ).astype(jnp.bfloat16)

    def line_peer(t):
        h, other = PEERS[t]
        return ((s // 2 + h + 8) % 8) * 2 + (s + other) % 2

    def for_peers(go):
        for t in range(NS - 1):
            go(t, 0)

    rows_s = pl.ds(pl.multiple_of(s * SUB, SUB), SUB)

    def line_ends(n, to):
        which, p, q0, q1 = UNITS[n]
        parts = pl.ds(q0, q1 - q0)
        if which == 0:
            there = x + to % 2 * (y - x)
            return send_l.at[to, p, parts], left_g.at[p, there, parts, rows_s]
        return send_r.at[to, p, parts], land_r.at[p, parts, rows_s]

    def line_copy(n, t):
        to = line_peer(t)
        src, dst = line_ends(n, to)
        return pltpu.make_async_remote_copy(
            src_ref=src, dst_ref=dst, send_sem=zs.at[n], recv_sem=zr.at[n],
            device_id=dev(f, to), device_id_type=MESH,
        )

    def norm_piece(p):
        at = pl.ds(p * SUB, SUB)
        values = x_ref[at].reshape(SUB * BLK, W).astype(jnp.float32)
        ready[at] = unit_channels(values, in_gain[...]).astype(jnp.bfloat16).reshape(SUB, BLK, W)

    def factor_piece(which, p):
        r = ready[pl.ds(p * SUB, SUB)].reshape(SUB * BLK, W)
        weight, stride, buf = ((left_w[...], 8, send_l), (right_mix, 1, send_r))[which]
        full = jnp.dot(r, weight, preferred_element_type=jnp.float32)
        full = full.astype(jnp.bfloat16).reshape(SUB, BLK, W)
        slabs = butterfly([full[i] for i in range(SUB)], stride)
        for i in range(SUB):
            buf[i, p] = slabs[i].reshape(NQ, SUB, W)

    def send(n):
        src, dst = line_ends(n, s)
        pltpu.make_async_copy(src, dst, zr.at[n]).start()

        def go(t, carry):
            line_copy(n, t).start()
            return carry

        for_peers(go)

    def gate_rows(i, carry):
        at = pl.multiple_of(i * SUB, SUB)
        r = ready[pl.ds(at, SUB)].reshape(SUB * BLK, W)
        g = jax.nn.sigmoid(jnp.dot(r, out_gate[...], preferred_element_type=jnp.float32))
        gate[pl.ds(at, SUB)] = g.reshape(SUB, BLK, W)
        return carry

    loads[1].wait()
    loads[2].wait()
    loads[3].wait()
    with jax.named_scope("factor"):
        norm_piece(0)
        factor_piece(0, 0)
    with jax.named_scope("barrier"):
        pl.semaphore_wait(barrier, (NS - 1) + 5)
    with jax.named_scope("send"):
        done = {(0, 0)}
        for n, (which, p, q0, q1) in enumerate(UNITS):
            if (which, p) not in done:
                if (1 - which, p) not in done:
                    if p == 1:
                        loads[4].wait()
                    norm_piece(p)
                factor_piece(which, p)
                done.add((which, p))
            send(n)
    for load in loads[5:]:
        load.wait()
    with jax.named_scope("gate"):
        lax.fori_loop(0, NP, gate_rows, 0)

    def ring_part(n, blocks, half=None):
        which, p, q0, q1 = UNITS[n]
        parts = q1 - q0
        if which == 0:
            rows_ = pl.ds(0, PART) if half is None else pl.ds(half * (PART // 2), PART // 2)
            return left_g.at[p, blocks, pl.ds(q0, parts), rows_]
        rows_ = pl.ds(0, W) if half is None else pl.ds(half * (W // 2), W // 2)
        return right_g.at[p, blocks, rows_, pl.ds(q0 * PART, parts * PART)]

    def ring_copy(n, block, half, step, sem):
        ref = ring_part(n, block, half)
        return pltpu.make_async_remote_copy(
            src_ref=ref, dst_ref=ref, send_sem=gs.at[n], recv_sem=gr.at[n, sem],
            device_id=dev(ring(UNITS[n][0], step), s), device_id_type=MESH,
        )

    def wait_for(ref, sem):
        pltpu.make_async_copy(ref, ref, sem).wait()

    def gather(n):
        which, p, q0, q1 = UNITS[n]
        parts = pl.ds(q0, q1 - q0)
        with jax.named_scope(f"line{n}"):
            wait_for(left_g.at[p, slot[0], parts] if which == 0 else land_r.at[p, parts], zr.at[n])
        if which == 1:
            with jax.named_scope(f"turn{n}"):
                block = land_r[p, q0:q1].reshape((q1 - q0) * PART, W)
                right_g[p, slot[1], :, q0 * PART : q1 * PART] = jnp.transpose(block)
        me = slot[which]
        ring_copy(n, me, 0, 1, 0).start()
        ring_copy(n, me, 1, NX - 1, 1).start()
        ring_copy(n, me, 1, 1, 2).start()
        ring_copy(n, me, 0, NX - 1, 2).start()

    def pass_on(n):
        me = slot[UNITS[n][0]]
        with jax.named_scope(f"pass{n}"):
            wait_for(ring_part(n, 0, 0), gr.at[n, 0])
            ring_copy(n, (me + NX - 1) % NX, 0, 1, 2).start()
            wait_for(ring_part(n, 0, 1), gr.at[n, 1])
            ring_copy(n, (me + 1) % NX, 1, NX - 1, 2).start()

    def gathered(n):
        with jax.named_scope(f"gathered{n}"):
            wait_for(ring_part(n, pl.ds(0, 2)), gr.at[n, 2])

    lane_channel = lax.broadcasted_iota(jnp.int32, (SUB, W), 1) % 8

    def product(a, b):
        with jax.named_scope(f"prod{a}{b}"):
            right = right_g[b].reshape(NY * W, KALL)
            for h in range(2):
                left = jnp.concatenate(
                    [left_g[a, 2 * h + u].reshape(KALL, W) for u in range(2)], axis=1
                )
                full = jnp.dot(right, left, preferred_element_type=jnp.float32)
                for v in range(NY):
                    for u in range(2):
                        tile = full[v * W : (v + 1) * W, u * W : (u + 1) * W]
                        res = tile[:SUB]
                        for d in range(1, 8):
                            res = jnp.where(lane_channel == d, tile[d * SUB : (d + 1) * SUB], res)
                        res = (res * KALL ** (-0.5)).astype(jnp.bfloat16)
                        stage[2 * h + u, b, a, v] = res

    def hop_copy(a, b, step):
        to = (slot[0] + step) % NX
        return pltpu.make_async_remote_copy(
            src_ref=stage.at[to, b, a], dst_ref=middle.at[slot[0], b, a],
            send_sem=hs.at[b, a], recv_sem=hr.at[b, a],
            device_id=dev(ring(0, step), s), device_id_type=MESH,
        )

    def hop(a, b):
        for step in (2, 1, 3):
            hop_copy(a, b, step).start()
        spread_from(0, a, b)

    group, place = pick(s % NX, s // NX), pick(s // NX, s % NX)

    def spread_from(ahead, a, b):
        w = (slot[0] + ahead) % NX

        for k in (1, 2, 3, 0):
            v = (place + k) % NY
            to = pick(v * NX + w, w * NX + v)
            src, dst = (stage.at[w, b, a, v] if ahead == 0 else middle.at[w, b, a, v]), land_o.at[s, b, a]

            def far(src=src, dst=dst, to=to):
                pltpu.make_async_remote_copy(
                    src_ref=src, dst_ref=dst, send_sem=os_.at[b, a], recv_sem=or_.at[b, a],
                    device_id=dev(f, to), device_id_type=MESH,
                ).start()

            if k:
                far()
                continue

            pl.when(w != group)(far)

            @pl.when(w == group)
            def _(src=src, dst=dst):
                pltpu.make_async_copy(src, dst, or_.at[b, a]).start()

    def spread(a, b):
        with jax.named_scope(f"hopwait{a}{b}"):
            ref = middle.at[pl.ds(0, 3), b, a]
            pltpu.make_async_copy(ref, ref, hr.at[b, a]).wait()
        with jax.named_scope(f"spread{a}{b}"):
            for ahead in AHEAD:
                spread_from(ahead, a, b)

    def arrived(a, b):
        ref = land_o.at[:, b, a]
        with jax.named_scope(f"arrive{a}{b}"):
            pltpu.make_async_copy(ref, ref, or_.at[b, a]).wait()

    def finish(tiles):
        with jax.named_scope("fin" + "_".join(f"{a}{b}" for a, b in tiles)):
            slabs = butterfly(
                [jnp.concatenate([land_o[i, b, a] for a, b in tiles], axis=0) for i in range(NS)], 8
            )
            mixed = jnp.concatenate(slabs, axis=0).astype(jnp.float32)
            scaled = unit_channels(mixed, mid_gain[...]).astype(jnp.bfloat16)
            res = jnp.dot(scaled, out_w[...], preferred_element_type=jnp.float32)
            res = res.reshape(SUB, len(tiles), SUB, W)
            for t, (a, b) in enumerate(tiles):
                rows_, at = pl.ds(a * SUB, SUB), pl.ds(b * SUB, SUB)
                o_ref[rows_, at] = (res[:, t] * gate[rows_, at]).astype(jnp.bfloat16)

    def make(a, b):
        product(a, b)
        hop(a, b)

    def end(*tiles):
        for a, b in tiles:
            arrived(a, b)
        finish(tiles)

    def drain_tiles(tiles):
        for a, b in tiles:
            wait_for(middle.at[pl.ds(0, 3), b, a], hs.at[b, a])
            wait_for(land_o.at[pl.ds(0, NS - 1), b, a], os_.at[b, a])

    def drain():
        for n, (which, p, q0, q1) in enumerate(UNITS):
            wait_for((send_l, send_r)[which].at[pl.ds(0, NS - 1), p, pl.ds(q0, q1 - q0)], zs.at[n])
            wait_for(ring_part(n, pl.ds(0, 3)), gs.at[n])
        drain_tiles(((0, 0), (1, 0), (0, 1), (1, 1), (2, 0)))

    gather(0)
    gather(1)
    pass_on(0)
    gather(2)
    pass_on(1)
    gathered(0)
    gather(3)
    pass_on(2)
    gathered(1)
    make(0, 0)
    gather(4)
    pass_on(3)
    gathered(2)
    make(1, 0)
    gather(5)
    spread(0, 0)
    gather(6)
    pass_on(4)
    gathered(3)
    make(0, 1)
    make(1, 1)
    pass_on(5)
    spread(1, 0)
    pass_on(6)
    gathered(4)
    make(2, 0)
    spread(0, 1)
    make(2, 1)
    spread(1, 1)
    gathered(5)
    gathered(6)
    make(0, 2)
    make(1, 2)
    make(2, 2)
    spread(2, 0)
    spread(2, 1)
    end((0, 0), (1, 0))
    spread(0, 2)
    spread(1, 2)
    spread(2, 2)
    end((0, 1), (1, 1))
    end((2, 0), (2, 1))
    drain()
    end((0, 2), (1, 2))
    end((2, 2))

    drain_tiles(((2, 1), (0, 2), (1, 2), (2, 2)))


def per_device(pair_state, in_gain, left_weight, right_weight, mid_gain, out_weight, out_gate):
    bf = jnp.bfloat16
    vmem = pl.BlockSpec(memory_space=pltpu.VMEM)
    return pl.pallas_call(
        kernel,
        out_shape=jax.ShapeDtypeStruct((BLK, BLK, W), bf),
        in_specs=[pl.BlockSpec(memory_space=pltpu.HBM)] * 7,
        out_specs=vmem,
        scratch_shapes=[
            pltpu.VMEM((BLK, BLK, W), bf),
            pltpu.VMEM((1, W), jnp.float32),
            pltpu.VMEM((W, W), bf),
            pltpu.VMEM((W, W), bf),
            pltpu.VMEM((1, W), jnp.float32),
            pltpu.VMEM((W, W), bf),
            pltpu.VMEM((W, W), bf),
            pltpu.SemaphoreType.DMA((8,)),
            pltpu.VMEM((BLK, BLK, W), bf),
            pltpu.VMEM((BLK, BLK, W), jnp.float32),
            pltpu.VMEM((NS, NP, NQ, SUB, W), bf),
            pltpu.VMEM((NS, NP, NQ, SUB, W), bf),
            pltpu.VMEM((NP, NQ, PART, W), bf),
            pltpu.VMEM((NP, NX, NQ, PART, W), bf),
            pltpu.VMEM((NP, NY, W, KALL), bf),
            pltpu.VMEM((NX, NP, NP, NY, SUB, W), bf),
            pltpu.VMEM((NX, NP, NP, NY, SUB, W), bf),
            pltpu.VMEM((NS, NP, NP, SUB, W), bf),
            pltpu.SemaphoreType.DMA((len(UNITS),)),
            pltpu.SemaphoreType.DMA((len(UNITS),)),
            pltpu.SemaphoreType.DMA((len(UNITS),)),
            pltpu.SemaphoreType.DMA((len(UNITS), 3)),
            pltpu.SemaphoreType.DMA((NP, NP)),
            pltpu.SemaphoreType.DMA((NP, NP)),
            pltpu.SemaphoreType.DMA((NP, NP)),
            pltpu.SemaphoreType.DMA((NP, NP)),
        ],
        compiler_params=pltpu.CompilerParams(
            collective_id=0, has_side_effects=True, vmem_limit_bytes=50_331_648
        ),
    )(*(pltpu.with_memory_space_constraint(v, pltpu.HBM) for v in (pair_state, in_gain.reshape(1, W), left_weight, right_weight, mid_gain.reshape(1, W), out_weight, out_gate)))


def solution(mesh):
    in_specs = (P("first", "second", None), P(), P(), P(), P(), P(), P())
    out_specs = P("first", "second", None)
    return jax.shard_map(
        per_device, mesh=mesh, in_specs=in_specs, out_specs=out_specs, check_vma=False
    )
```

```python
import functools

import jax
import jax.numpy as jnp
from jax import lax
from jax.experimental import pallas as pl
from jax.experimental.pallas import tpu as pltpu
from jax.sharding import PartitionSpec as P

MESH = pl.DeviceIdType.MESH
NX, NY, NS = 4, 4, 16
BLK = 48
SUB = 16
NP = BLK // SUB
W = 128
KALL = BLK * NS
NQ = BLK // SUB
PART = NS * SUB
UNITS = (
    (0, 0, 0, 3),
    (1, 0, 0, 3),
    (0, 1, 0, 3),
    (1, 1, 0, 3),
    (0, 2, 0, 3),
    (1, 2, 0, 2),
    (1, 2, 2, 3),
)


PEERS = tuple((h, other) for other in (0, 1) for h in (4, 3, -3, 2, -2, 1, -1, 0) if (h, other) != (0, 0))


AHEAD = (3, 1, 2)


def unit_channels(values, channel_gain):
    centred = values - jnp.mean(values, axis=-1, keepdims=True)
    return (
        centred
        * lax.rsqrt(jnp.mean(centred * centred, axis=-1, keepdims=True) + 1e-05)
        * channel_gain
    )


def butterfly(slabs, first_stride):
    n = len(slabs)
    lane = lax.broadcasted_iota(jnp.int32, slabs[0].shape, 1)
    bit = 1
    while bit < n:
        stride = bit * first_stride
        low = (lane // stride) % 2 == 0
        out = list(slabs)
        for a in range(n):
            if a & bit:
                continue
            b = a | bit
            u, v = slabs[a], slabs[b]
            out[a] = jnp.where(low, u, pltpu.roll(v, stride, 1))
            out[b] = jnp.where(low, pltpu.roll(u, W - stride, 1), v)
        slabs = out
        bit *= 2
    return slabs


def kernel(
    x_hbm, in_gain_hbm, left_hbm, right_hbm, mid_gain_hbm, out_hbm, gate_hbm,
    o_ref,
    x_ref, in_gain, left_w, right_w, mid_gain, out_w, out_gate, ls,
    ready, gate, send_l, send_r, land_r, left_g, right_g, stage, middle, land_o,
    zs, zr, gs, gr, hs, hr, os_, or_,
):
    f, s = lax.axis_index("first"), lax.axis_index("second")
    y, x = f // NX, f % NX

    def dev(first, second):
        return {"first": first, "second": second}

    turned = s % 2

    def pick(straight, crossed):
        return straight + turned * (crossed - straight)

    slot = (pick(x, y), pick(y, x))

    def ring(which, step):
        along_x, along_y = y * NX + (x + step) % NX, (y + step) % NY * NX + x
        return pick(along_x, along_y) if which == 0 else pick(along_y, along_x)


    barrier = pltpu.get_barrier_semaphore()

    def greet(first, second):
        pl.semaphore_signal(barrier, inc=1, device_id=dev(first, second), device_id_type=MESH)

    def line_peer(t):
        h, other = PEERS[t]
        return ((s // 2 + h + 8) % 8) * 2 + (s + other) % 2

    def for_peers(go):
        for t in range(NS - 1):
            go(t, 0)

    for t in range(NS - 1):
        greet(f, line_peer(t))
    for step in (1, NX - 1):
        for which in (0, 1):
            greet(ring(which, step), s)
    greet(ring(0, 2), s)


    loads = [
        pltpu.make_async_copy(src, dst, ls.at[n])
        for n, (src, dst) in enumerate((
            (right_hbm, right_w), (in_gain_hbm, in_gain), (left_hbm, left_w),
            (x_hbm.at[pl.ds(0, SUB)], x_ref.at[pl.ds(0, SUB)]),
            (x_hbm.at[pl.ds(SUB, BLK - SUB)], x_ref.at[pl.ds(SUB, BLK - SUB)]),
            (gate_hbm, out_gate), (mid_gain_hbm, mid_gain), (out_hbm, out_w),
        ))
    ]
    for load in loads:
        load.start()

    rows = lax.broadcasted_iota(jnp.int32, (W, W), 0)
    cols = lax.broadcasted_iota(jnp.int32, (W, W), 1)
    swap = (rows == (cols % 16) * 8 + cols // 16).astype(jnp.bfloat16)
    loads[0].wait()
    right_mix = jnp.dot(
        right_w[...], swap, preferred_element_type=jnp.float32
    ).astype(jnp.bfloat16)

    rows_s = pl.ds(pl.multiple_of(s * SUB, SUB), SUB)

    def line_ends(n, to):
        which, p, q0, q1 = UNITS[n]
        parts = pl.ds(q0, q1 - q0)
        if which == 0:
            there = x + to % 2 * (y - x)
            return send_l.at[to, p, parts], left_g.at[p, there, parts, rows_s]
        return send_r.at[to, p, parts], land_r.at[p, parts, rows_s]

    def line_copy(n, t):
        to = line_peer(t)
        src, dst = line_ends(n, to)
        return pltpu.make_async_remote_copy(
            src_ref=src, dst_ref=dst, send_sem=zs.at[n], recv_sem=zr.at[n],
            device_id=dev(f, to), device_id_type=MESH,
        )

    def norm_piece(p):
        at = pl.ds(p * SUB, SUB)
        values = x_ref[at].reshape(SUB * BLK, W).astype(jnp.float32)
        ready[at] = unit_channels(values, in_gain[...]).astype(jnp.bfloat16).reshape(SUB, BLK, W)

    def factor_piece(which, p):
        r = ready[pl.ds(p * SUB, SUB)].reshape(SUB * BLK, W)
        weight, stride, buf = ((left_w[...], 8, send_l), (right_mix, 1, send_r))[which]
        full = jnp.dot(r, weight, preferred_element_type=jnp.float32)
        full = full.astype(jnp.bfloat16).reshape(SUB, BLK, W)
        slabs = butterfly([full[i] for i in range(SUB)], stride)
        for i in range(SUB):
            buf[i, p] = slabs[i].reshape(NQ, SUB, W)

    def send(n):
        src, dst = line_ends(n, s)
        pltpu.make_async_copy(src, dst, zr.at[n]).start()

        def go(t, carry):
            line_copy(n, t).start()
            return carry

        for_peers(go)

    def gate_rows(i, carry):
        at = pl.multiple_of(i * SUB, SUB)
        r = ready[pl.ds(at, SUB)].reshape(SUB * BLK, W)
        g = jax.nn.sigmoid(jnp.dot(r, out_gate[...], preferred_element_type=jnp.float32))
        gate[pl.ds(at, SUB)] = g.reshape(SUB, BLK, W)
        return carry

    loads[1].wait()
    loads[2].wait()
    loads[3].wait()
    with jax.named_scope("factor"):
        norm_piece(0)
        factor_piece(0, 0)
    with jax.named_scope("barrier"):
        pl.semaphore_wait(barrier, (NS - 1) + 5)
    with jax.named_scope("send"):
        done = {(0, 0)}
        for n, (which, p, q0, q1) in enumerate(UNITS):
            if (which, p) not in done:
                if (1 - which, p) not in done:
                    if p == 1:
                        loads[4].wait()
                    norm_piece(p)
                factor_piece(which, p)
                done.add((which, p))
            send(n)
    for load in loads[5:]:
        load.wait()
    with jax.named_scope("gate"):
        lax.fori_loop(0, NP, gate_rows, 0)

    def ring_part(n, blocks, half=None):
        which, p, q0, q1 = UNITS[n]
        parts = q1 - q0
        if which == 0:
            rows_ = pl.ds(0, PART) if half is None else pl.ds(half * (PART // 2), PART // 2)
            return left_g.at[p, blocks, pl.ds(q0, parts), rows_]
        rows_ = pl.ds(0, W) if half is None else pl.ds(half * (W // 2), W // 2)
        return right_g.at[p, blocks, rows_, pl.ds(q0 * PART, parts * PART)]

    def ring_copy(n, block, half, step, sem):
        ref = ring_part(n, block, half)
        return pltpu.make_async_remote_copy(
            src_ref=ref, dst_ref=ref, send_sem=gs.at[n], recv_sem=gr.at[n, sem],
            device_id=dev(ring(UNITS[n][0], step), s), device_id_type=MESH,
        )

    def wait_for(ref, sem):
        pltpu.make_async_copy(ref, ref, sem).wait()

    def gather(n):
        which, p, q0, q1 = UNITS[n]
        parts = pl.ds(q0, q1 - q0)
        with jax.named_scope(f"line{n}"):
            wait_for(left_g.at[p, slot[0], parts] if which == 0 else land_r.at[p, parts], zr.at[n])
        if which == 1:
            with jax.named_scope(f"turn{n}"):
                block = land_r[p, q0:q1].reshape((q1 - q0) * PART, W)
                right_g[p, slot[1], :, q0 * PART : q1 * PART] = jnp.transpose(block)
        me = slot[which]
        ring_copy(n, me, 0, 1, 0).start()
        ring_copy(n, me, 1, NX - 1, 1).start()
        ring_copy(n, me, 1, 1, 2).start()
        ring_copy(n, me, 0, NX - 1, 2).start()

    def pass_on(n):
        me = slot[UNITS[n][0]]
        with jax.named_scope(f"pass{n}"):
            wait_for(ring_part(n, 0, 0), gr.at[n, 0])
            ring_copy(n, (me + NX - 1) % NX, 0, 1, 2).start()
            wait_for(ring_part(n, 0, 1), gr.at[n, 1])
            ring_copy(n, (me + 1) % NX, 1, NX - 1, 2).start()

    def gathered(n):
        with jax.named_scope(f"gathered{n}"):
            wait_for(ring_part(n, pl.ds(0, 2)), gr.at[n, 2])

    lane_channel = lax.broadcasted_iota(jnp.int32, (SUB, W), 1) % 8

    def product(a, b):
        with jax.named_scope(f"prod{a}{b}"):
            right = right_g[b].reshape(NY * W, KALL)
            for h in range(2):
                left = jnp.concatenate(
                    [left_g[a, 2 * h + u].reshape(KALL, W) for u in range(2)], axis=1
                )
                full = jnp.dot(right, left, preferred_element_type=jnp.float32)
                for v in range(NY):
                    for u in range(2):
                        tile = full[v * W : (v + 1) * W, u * W : (u + 1) * W]
                        res = tile[:SUB]
                        for d in range(1, 8):
                            res = jnp.where(lane_channel == d, tile[d * SUB : (d + 1) * SUB], res)
                        res = (res * KALL ** (-0.5)).astype(jnp.bfloat16)
                        stage[2 * h + u, b, a, v] = res

    def hop_copy(a, b, step):
        to = (slot[0] + step) % NX
        return pltpu.make_async_remote_copy(
            src_ref=stage.at[to, b, a], dst_ref=middle.at[slot[0], b, a],
            send_sem=hs.at[b, a], recv_sem=hr.at[b, a],
            device_id=dev(ring(0, step), s), device_id_type=MESH,
        )

    def hop(a, b):
        for step in (2, 1, 3):
            hop_copy(a, b, step).start()
        spread_from(0, a, b)

    group, place = pick(s % NX, s // NX), pick(s // NX, s % NX)

    def spread_from(ahead, a, b):
        w = (slot[0] + ahead) % NX

        for k in (1, 2, 3, 0):
            v = (place + k) % NY
            to = pick(v * NX + w, w * NX + v)
            src, dst = (stage.at[w, b, a, v] if ahead == 0 else middle.at[w, b, a, v]), land_o.at[s, b, a]

            def far(src=src, dst=dst, to=to):
                pltpu.make_async_remote_copy(
                    src_ref=src, dst_ref=dst, send_sem=os_.at[b, a], recv_sem=or_.at[b, a],
                    device_id=dev(f, to), device_id_type=MESH,
                ).start()

            if k:
                far()
                continue

            pl.when(w != group)(far)

            @pl.when(w == group)
            def _(src=src, dst=dst):
                pltpu.make_async_copy(src, dst, or_.at[b, a]).start()

    def spread(a, b):
        with jax.named_scope(f"hopwait{a}{b}"):
            ref = middle.at[pl.ds(0, 3), b, a]
            pltpu.make_async_copy(ref, ref, hr.at[b, a]).wait()
        with jax.named_scope(f"spread{a}{b}"):
            for ahead in AHEAD:
                spread_from(ahead, a, b)

    def arrived(a, b):
        ref = land_o.at[:, b, a]
        with jax.named_scope(f"arrive{a}{b}"):
            pltpu.make_async_copy(ref, ref, or_.at[b, a]).wait()

    def finish(tiles):
        with jax.named_scope("fin" + "_".join(f"{a}{b}" for a, b in tiles)):
            slabs = butterfly(
                [jnp.concatenate([land_o[i, b, a] for a, b in tiles], axis=0) for i in range(NS)], 8
            )
            mixed = jnp.concatenate(slabs, axis=0).astype(jnp.float32)
            scaled = unit_channels(mixed, mid_gain[...]).astype(jnp.bfloat16)
            res = jnp.dot(scaled, out_w[...], preferred_element_type=jnp.float32)
            res = res.reshape(SUB, len(tiles), SUB, W)
            for t, (a, b) in enumerate(tiles):
                rows_, at = pl.ds(a * SUB, SUB), pl.ds(b * SUB, SUB)
                o_ref[rows_, at] = (res[:, t] * gate[rows_, at]).astype(jnp.bfloat16)

    def make(a, b):
        product(a, b)
        hop(a, b)

    def end(*tiles):
        for a, b in tiles:
            arrived(a, b)
        finish(tiles)

    def drain_tiles(tiles):
        for a, b in tiles:
            wait_for(middle.at[pl.ds(0, 3), b, a], hs.at[b, a])
            wait_for(land_o.at[pl.ds(0, NS - 1), b, a], os_.at[b, a])

    def drain():
        for n, (which, p, q0, q1) in enumerate(UNITS):
            wait_for((send_l, send_r)[which].at[pl.ds(0, NS - 1), p, pl.ds(q0, q1 - q0)], zs.at[n])
            wait_for(ring_part(n, pl.ds(0, 3)), gs.at[n])
        drain_tiles(((0, 0), (1, 0), (0, 1), (1, 1), (2, 0)))

    gather(0)
    gather(1)
    pass_on(0)
    gather(2)
    pass_on(1)
    gathered(0)
    gather(3)
    pass_on(2)
    gathered(1)
    make(0, 0)
    gather(4)
    pass_on(3)
    gathered(2)
    make(1, 0)
    gather(5)
    spread(0, 0)
    gather(6)
    pass_on(4)
    gathered(3)
    make(0, 1)
    make(1, 1)
    pass_on(5)
    spread(1, 0)
    pass_on(6)
    gathered(4)
    make(2, 0)
    spread(0, 1)
    make(2, 1)
    spread(1, 1)
    gathered(5)
    gathered(6)
    make(0, 2)
    make(1, 2)
    make(2, 2)
    spread(2, 0)
    spread(2, 1)
    end((0, 0), (1, 0))
    spread(0, 2)
    spread(1, 2)
    spread(2, 2)
    end((0, 1), (1, 1))
    drain()
    end((2, 0), (2, 1))
    end((0, 2))
    end((1, 2), (2, 2))

    drain_tiles(((2, 1), (0, 2), (1, 2), (2, 2)))


def per_device(pair_state, in_gain, left_weight, right_weight, mid_gain, out_weight, out_gate):
    bf = jnp.bfloat16
    vmem = pl.BlockSpec(memory_space=pltpu.VMEM)
    return pl.pallas_call(
        kernel,
        out_shape=jax.ShapeDtypeStruct((BLK, BLK, W), bf),
        in_specs=[pl.BlockSpec(memory_space=pltpu.HBM)] * 7,
        out_specs=vmem,
        scratch_shapes=[
            pltpu.VMEM((BLK, BLK, W), bf),
            pltpu.VMEM((1, W), jnp.float32),
            pltpu.VMEM((W, W), bf),
            pltpu.VMEM((W, W), bf),
            pltpu.VMEM((1, W), jnp.float32),
            pltpu.VMEM((W, W), bf),
            pltpu.VMEM((W, W), bf),
            pltpu.SemaphoreType.DMA((8,)),
            pltpu.VMEM((BLK, BLK, W), bf),
            pltpu.VMEM((BLK, BLK, W), jnp.float32),
            pltpu.VMEM((NS, NP, NQ, SUB, W), bf),
            pltpu.VMEM((NS, NP, NQ, SUB, W), bf),
            pltpu.VMEM((NP, NQ, PART, W), bf),
            pltpu.VMEM((NP, NX, NQ, PART, W), bf),
            pltpu.VMEM((NP, NY, W, KALL), bf),
            pltpu.VMEM((NX, NP, NP, NY, SUB, W), bf),
            pltpu.VMEM((NX, NP, NP, NY, SUB, W), bf),
            pltpu.VMEM((NS, NP, NP, SUB, W), bf),
            pltpu.SemaphoreType.DMA((len(UNITS),)),
            pltpu.SemaphoreType.DMA((len(UNITS),)),
            pltpu.SemaphoreType.DMA((len(UNITS),)),
            pltpu.SemaphoreType.DMA((len(UNITS), 3)),
            pltpu.SemaphoreType.DMA((NP, NP)),
            pltpu.SemaphoreType.DMA((NP, NP)),
            pltpu.SemaphoreType.DMA((NP, NP)),
            pltpu.SemaphoreType.DMA((NP, NP)),
        ],
        compiler_params=pltpu.CompilerParams(
            collective_id=0, has_side_effects=True, vmem_limit_bytes=50_331_648
        ),
    )(*(pltpu.with_memory_space_constraint(v, pltpu.HBM) for v in (pair_state, in_gain.reshape(1, W), left_weight, right_weight, mid_gain.reshape(1, W), out_weight, out_gate)))


def solution(mesh):
    in_specs = (P("first", "second", None), P(), P(), P(), P(), P(), P())
    out_specs = P("first", "second", None)
    return jax.shard_map(
        per_device, mesh=mesh, in_specs=in_specs, out_specs=out_specs, check_vma=False
    )
```

```python
import functools

import jax
import jax.numpy as jnp
from jax import lax
from jax.experimental import pallas as pl
from jax.experimental.pallas import tpu as pltpu
from jax.sharding import PartitionSpec as P

MESH = pl.DeviceIdType.MESH
NX, NY, NS = 4, 4, 16
BLK = 48
SUB = 16
NP = BLK // SUB
W = 128
KALL = BLK * NS
NQ = BLK // SUB
PART = NS * SUB
UNITS = (
    (0, 0, 0, 3),
    (1, 0, 0, 3),
    (0, 1, 0, 3),
    (1, 1, 0, 3),
    (0, 2, 0, 3),
    (1, 2, 0, 2),
    (1, 2, 2, 3),
)


PEERS = tuple((h, other) for other in (0, 1) for h in (4, 3, -3, 2, -2, 1, -1, 0) if (h, other) != (0, 0))


AHEAD = (3, 1, 2)


def unit_channels(values, channel_gain):
    centred = values - jnp.mean(values, axis=-1, keepdims=True)
    return (
        centred
        * lax.rsqrt(jnp.mean(centred * centred, axis=-1, keepdims=True) + 1e-05)
        * channel_gain
    )


def butterfly(slabs, first_stride):
    n = len(slabs)
    lane = lax.broadcasted_iota(jnp.int32, slabs[0].shape, 1)
    bit = 1
    while bit < n:
        stride = bit * first_stride
        low = (lane // stride) % 2 == 0
        out = list(slabs)
        for a in range(n):
            if a & bit:
                continue
            b = a | bit
            u, v = slabs[a], slabs[b]
            out[a] = jnp.where(low, u, pltpu.roll(v, stride, 1))
            out[b] = jnp.where(low, pltpu.roll(u, W - stride, 1), v)
        slabs = out
        bit *= 2
    return slabs


def kernel(
    x_hbm, in_gain_hbm, left_hbm, right_hbm, mid_gain_hbm, out_hbm, gate_hbm,
    o_ref,
    x_ref, in_gain, left_w, right_w, mid_gain, out_w, out_gate, ls,
    ready, gate, send_l, send_r, land_r, left_g, right_g, stage, middle, land_o,
    zs, zr, gs, gr, hs, hr, os_, or_,
):
    f, s = lax.axis_index("first"), lax.axis_index("second")
    y, x = f // NX, f % NX

    def dev(first, second):
        return {"first": first, "second": second}

    turned = s % 2

    def pick(straight, crossed):
        return straight + turned * (crossed - straight)

    slot = (pick(x, y), pick(y, x))

    def ring(which, step):
        along_x, along_y = y * NX + (x + step) % NX, (y + step) % NY * NX + x
        return pick(along_x, along_y) if which == 0 else pick(along_y, along_x)


    barrier = pltpu.get_barrier_semaphore()

    def greet(first, second):
        pl.semaphore_signal(barrier, inc=1, device_id=dev(first, second), device_id_type=MESH)

    def line_peer(t):
        h, other = PEERS[t]
        return ((s // 2 + h + 8) % 8) * 2 + (s + other) % 2

    def for_peers(go):
        for t in range(NS - 1):
            go(t, 0)

    for t in range(NS - 1):
        greet(f, line_peer(t))
    for step in (1, NX - 1):
        for which in (0, 1):
            greet(ring(which, step), s)
    greet(ring(0, 2), s)


    loads = [
        pltpu.make_async_copy(src, dst, ls.at[n])
        for n, (src, dst) in enumerate((
            (right_hbm, right_w), (in_gain_hbm, in_gain), (left_hbm, left_w),
            (x_hbm.at[pl.ds(0, SUB)], x_ref.at[pl.ds(0, SUB)]),
            (x_hbm.at[pl.ds(SUB, BLK - SUB)], x_ref.at[pl.ds(SUB, BLK - SUB)]),
            (gate_hbm, out_gate), (mid_gain_hbm, mid_gain), (out_hbm, out_w),
        ))
    ]
    for load in loads:
        load.start()

    rows = lax.broadcasted_iota(jnp.int32, (W, W), 0)
    cols = lax.broadcasted_iota(jnp.int32, (W, W), 1)
    swap = (rows == (cols % 16) * 8 + cols // 16).astype(jnp.bfloat16)
    loads[0].wait()
    right_mix = jnp.dot(
        right_w[...], swap, preferred_element_type=jnp.float32
    ).astype(jnp.bfloat16)

    rows_s = pl.ds(pl.multiple_of(s * SUB, SUB), SUB)

    def line_ends(n, to):
        which, p, q0, q1 = UNITS[n]
        parts = pl.ds(q0, q1 - q0)
        if which == 0:
            there = x + to % 2 * (y - x)
            return send_l.at[to, p, parts], left_g.at[p, there, parts, rows_s]
        return send_r.at[to, p, parts], land_r.at[p, parts, rows_s]

    def line_copy(n, t):
        to = line_peer(t)
        src, dst = line_ends(n, to)
        return pltpu.make_async_remote_copy(
            src_ref=src, dst_ref=dst, send_sem=zs.at[n], recv_sem=zr.at[n],
            device_id=dev(f, to), device_id_type=MESH,
        )

    def norm_piece(p):
        at = pl.ds(p * SUB, SUB)
        values = x_ref[at].reshape(SUB * BLK, W).astype(jnp.float32)
        ready[at] = unit_channels(values, in_gain[...]).astype(jnp.bfloat16).reshape(SUB, BLK, W)

    def factor_piece(which, p):
        r = ready[pl.ds(p * SUB, SUB)].reshape(SUB * BLK, W)
        weight, stride, buf = ((left_w[...], 8, send_l), (right_mix, 1, send_r))[which]
        full = jnp.dot(r, weight, preferred_element_type=jnp.float32)
        full = full.astype(jnp.bfloat16).reshape(SUB, BLK, W)
        slabs = butterfly([full[i] for i in range(SUB)], stride)
        for i in range(SUB):
            buf[i, p] = slabs[i].reshape(NQ, SUB, W)

    def send(n):
        src, dst = line_ends(n, s)
        pltpu.make_async_copy(src, dst, zr.at[n]).start()

        def go(t, carry):
            line_copy(n, t).start()
            return carry

        for_peers(go)

    def gate_rows(i, carry):
        at = pl.multiple_of(i * SUB, SUB)
        r = ready[pl.ds(at, SUB)].reshape(SUB * BLK, W)
        g = jax.nn.sigmoid(jnp.dot(r, out_gate[...], preferred_element_type=jnp.float32))
        gate[pl.ds(at, SUB)] = g.reshape(SUB, BLK, W)
        return carry

    loads[1].wait()
    loads[2].wait()
    loads[3].wait()
    with jax.named_scope("factor"):
        norm_piece(0)
        factor_piece(0, 0)
    with jax.named_scope("barrier"):
        pl.semaphore_wait(barrier, (NS - 1) + 5)
    with jax.named_scope("send"):
        done = {(0, 0)}
        for n, (which, p, q0, q1) in enumerate(UNITS):
            if (which, p) not in done:
                if (1 - which, p) not in done:
                    if p == 1:
                        loads[4].wait()
                    norm_piece(p)
                factor_piece(which, p)
                done.add((which, p))
            send(n)
    for load in loads[5:]:
        load.wait()
    with jax.named_scope("gate"):
        lax.fori_loop(0, NP, gate_rows, 0)

    def ring_part(n, blocks, half=None):
        which, p, q0, q1 = UNITS[n]
        parts = q1 - q0
        if which == 0:
            rows_ = pl.ds(0, PART) if half is None else pl.ds(half * (PART // 2), PART // 2)
            return left_g.at[p, blocks, pl.ds(q0, parts), rows_]
        rows_ = pl.ds(0, W) if half is None else pl.ds(half * (W // 2), W // 2)
        return right_g.at[p, blocks, rows_, pl.ds(q0 * PART, parts * PART)]

    def ring_copy(n, block, half, step, sem):
        ref = ring_part(n, block, half)
        return pltpu.make_async_remote_copy(
            src_ref=ref, dst_ref=ref, send_sem=gs.at[n], recv_sem=gr.at[n, sem],
            device_id=dev(ring(UNITS[n][0], step), s), device_id_type=MESH,
        )

    def wait_for(ref, sem):
        pltpu.make_async_copy(ref, ref, sem).wait()

    def gather(n):
        which, p, q0, q1 = UNITS[n]
        parts = pl.ds(q0, q1 - q0)
        with jax.named_scope(f"line{n}"):
            wait_for(left_g.at[p, slot[0], parts] if which == 0 else land_r.at[p, parts], zr.at[n])
        if which == 1:
            with jax.named_scope(f"turn{n}"):
                block = land_r[p, q0:q1].reshape((q1 - q0) * PART, W)
                right_g[p, slot[1], :, q0 * PART : q1 * PART] = jnp.transpose(block)
        me = slot[which]
        ring_copy(n, me, 0, 1, 0).start()
        ring_copy(n, me, 1, NX - 1, 1).start()
        ring_copy(n, me, 1, 1, 2).start()
        ring_copy(n, me, 0, NX - 1, 2).start()

    def pass_on(n):
        me = slot[UNITS[n][0]]
        with jax.named_scope(f"pass{n}"):
            wait_for(ring_part(n, 0, 0), gr.at[n, 0])
            ring_copy(n, (me + NX - 1) % NX, 0, 1, 2).start()
            wait_for(ring_part(n, 0, 1), gr.at[n, 1])
            ring_copy(n, (me + 1) % NX, 1, NX - 1, 2).start()

    def gathered(n):
        with jax.named_scope(f"gathered{n}"):
            wait_for(ring_part(n, pl.ds(0, 2)), gr.at[n, 2])

    lane_channel = lax.broadcasted_iota(jnp.int32, (SUB, W), 1) % 8

    def product(a, b):
        with jax.named_scope(f"prod{a}{b}"):
            right = right_g[b].reshape(NY * W, KALL)
            for h in range(2):
                left = jnp.concatenate(
                    [left_g[a, 2 * h + u].reshape(KALL, W) for u in range(2)], axis=1
                )
                full = jnp.dot(right, left, preferred_element_type=jnp.float32)
                for v in range(NY):
                    for u in range(2):
                        tile = full[v * W : (v + 1) * W, u * W : (u + 1) * W]
                        res = tile[:SUB]
                        for d in range(1, 8):
                            res = jnp.where(lane_channel == d, tile[d * SUB : (d + 1) * SUB], res)
                        res = (res * KALL ** (-0.5)).astype(jnp.bfloat16)
                        stage[2 * h + u, b, a, v] = res

    def hop_copy(a, b, step):
        to = (slot[0] + step) % NX
        return pltpu.make_async_remote_copy(
            src_ref=stage.at[to, b, a], dst_ref=middle.at[slot[0], b, a],
            send_sem=hs.at[b, a], recv_sem=hr.at[b, a],
            device_id=dev(ring(0, step), s), device_id_type=MESH,
        )

    def hop(a, b):
        for step in (2, 1, 3):
            hop_copy(a, b, step).start()
        spread_from(0, a, b)

    group, place = pick(s % NX, s // NX), pick(s // NX, s % NX)

    def spread_from(ahead, a, b):
        w = (slot[0] + ahead) % NX

        for k in (1, 2, 3, 0):
            v = (place + k) % NY
            to = pick(v * NX + w, w * NX + v)
            src, dst = (stage.at[w, b, a, v] if ahead == 0 else middle.at[w, b, a, v]), land_o.at[s, b, a]

            def far(src=src, dst=dst, to=to):
                pltpu.make_async_remote_copy(
                    src_ref=src, dst_ref=dst, send_sem=os_.at[b, a], recv_sem=or_.at[b, a],
                    device_id=dev(f, to), device_id_type=MESH,
                ).start()

            if k:
                far()
                continue

            pl.when(w != group)(far)

            @pl.when(w == group)
            def _(src=src, dst=dst):
                pltpu.make_async_copy(src, dst, or_.at[b, a]).start()

    def spread(a, b):
        with jax.named_scope(f"hopwait{a}{b}"):
            ref = middle.at[pl.ds(0, 3), b, a]
            pltpu.make_async_copy(ref, ref, hr.at[b, a]).wait()
        with jax.named_scope(f"spread{a}{b}"):
            for ahead in AHEAD:
                spread_from(ahead, a, b)

    def arrived(a, b):
        ref = land_o.at[:, b, a]
        with jax.named_scope(f"arrive{a}{b}"):
            pltpu.make_async_copy(ref, ref, or_.at[b, a]).wait()

    def finish(tiles):
        with jax.named_scope("fin" + "_".join(f"{a}{b}" for a, b in tiles)):
            slabs = butterfly(
                [jnp.concatenate([land_o[i, b, a] for a, b in tiles], axis=0) for i in range(NS)], 8
            )
            mixed = jnp.concatenate(slabs, axis=0).astype(jnp.float32)
            scaled = unit_channels(mixed, mid_gain[...]).astype(jnp.bfloat16)
            res = jnp.dot(scaled, out_w[...], preferred_element_type=jnp.float32)
            res = res.reshape(SUB, len(tiles), SUB, W)
            for t, (a, b) in enumerate(tiles):
                rows_, at = pl.ds(a * SUB, SUB), pl.ds(b * SUB, SUB)
                o_ref[rows_, at] = (res[:, t] * gate[rows_, at]).astype(jnp.bfloat16)

    def make(a, b):
        product(a, b)
        hop(a, b)

    def end(*tiles):
        for a, b in tiles:
            arrived(a, b)
        finish(tiles)

    def drain_tiles(tiles):
        for a, b in tiles:
            wait_for(middle.at[pl.ds(0, 3), b, a], hs.at[b, a])
            wait_for(land_o.at[pl.ds(0, NS - 1), b, a], os_.at[b, a])

    def drain():
        for n, (which, p, q0, q1) in enumerate(UNITS):
            wait_for((send_l, send_r)[which].at[pl.ds(0, NS - 1), p, pl.ds(q0, q1 - q0)], zs.at[n])
            wait_for(ring_part(n, pl.ds(0, 3)), gs.at[n])
        drain_tiles(((0, 0), (1, 0), (0, 1), (1, 1), (2, 0)))

    gather(0)
    gather(1)
    pass_on(0)
    gather(2)
    pass_on(1)
    gathered(0)
    gather(3)
    pass_on(2)
    gathered(1)
    make(0, 0)
    gather(4)
    pass_on(3)
    gathered(2)
    make(1, 0)
    gather(5)
    spread(0, 0)
    gather(6)
    pass_on(4)
    gathered(3)
    make(0, 1)
    make(1, 1)
    pass_on(5)
    spread(1, 0)
    pass_on(6)
    spread(0, 1)
    gathered(4)
    make(2, 0)
    spread(1, 1)
    make(2, 1)
    gathered(5)
    gathered(6)
    make(0, 2)
    make(1, 2)
    make(2, 2)
    spread(2, 0)
    spread(2, 1)
    end((0, 0), (1, 0))
    spread(0, 2)
    spread(1, 2)
    spread(2, 2)
    end((0, 1), (1, 1))
    drain()
    end((2, 0), (2, 1))
    end((0, 2))
    end((1, 2), (2, 2))

    drain_tiles(((2, 1), (0, 2), (1, 2), (2, 2)))


def per_device(pair_state, in_gain, left_weight, right_weight, mid_gain, out_weight, out_gate):
    bf = jnp.bfloat16
    vmem = pl.BlockSpec(memory_space=pltpu.VMEM)
    return pl.pallas_call(
        kernel,
        out_shape=jax.ShapeDtypeStruct((BLK, BLK, W), bf),
        in_specs=[pl.BlockSpec(memory_space=pltpu.HBM)] * 7,
        out_specs=vmem,
        scratch_shapes=[
            pltpu.VMEM((BLK, BLK, W), bf),
            pltpu.VMEM((1, W), jnp.float32),
            pltpu.VMEM((W, W), bf),
            pltpu.VMEM((W, W), bf),
            pltpu.VMEM((1, W), jnp.float32),
            pltpu.VMEM((W, W), bf),
            pltpu.VMEM((W, W), bf),
            pltpu.SemaphoreType.DMA((8,)),
            pltpu.VMEM((BLK, BLK, W), bf),
            pltpu.VMEM((BLK, BLK, W), jnp.float32),
            pltpu.VMEM((NS, NP, NQ, SUB, W), bf),
            pltpu.VMEM((NS, NP, NQ, SUB, W), bf),
            pltpu.VMEM((NP, NQ, PART, W), bf),
            pltpu.VMEM((NP, NX, NQ, PART, W), bf),
            pltpu.VMEM((NP, NY, W, KALL), bf),
            pltpu.VMEM((NX, NP, NP, NY, SUB, W), bf),
            pltpu.VMEM((NX, NP, NP, NY, SUB, W), bf),
            pltpu.VMEM((NS, NP, NP, SUB, W), bf),
            pltpu.SemaphoreType.DMA((len(UNITS),)),
            pltpu.SemaphoreType.DMA((len(UNITS),)),
            pltpu.SemaphoreType.DMA((len(UNITS),)),
            pltpu.SemaphoreType.DMA((len(UNITS), 3)),
            pltpu.SemaphoreType.DMA((NP, NP)),
            pltpu.SemaphoreType.DMA((NP, NP)),
            pltpu.SemaphoreType.DMA((NP, NP)),
            pltpu.SemaphoreType.DMA((NP, NP)),
        ],
        compiler_params=pltpu.CompilerParams(
            collective_id=0, has_side_effects=True, vmem_limit_bytes=50_331_648
        ),
    )(*(pltpu.with_memory_space_constraint(v, pltpu.HBM) for v in (pair_state, in_gain.reshape(1, W), left_weight, right_weight, mid_gain.reshape(1, W), out_weight, out_gate)))


def solution(mesh):
    in_specs = (P("first", "second", None), P(), P(), P(), P(), P(), P())
    out_specs = P("first", "second", None)
    return jax.shard_map(
        per_device, mesh=mesh, in_specs=in_specs, out_specs=out_specs, check_vma=False
    )
```
